256 devices in a mesh: track: 4 (over y), ifg: 4 (over z_lo), pix: 16 (over z_hi, x, core).
Axes of the slice: x: 4, y: 4, z: 8 (z_hi: 2, z_lo: 4; z = z_hi * 4 + z_lo), core: 2. Of those that a mesh axis runs over, the one named last changes fastest.
Arguments:
- phases: bfloat16 [4, 600, 262144], P('track', 'ifg', 'pix')
- pairs: int32 [4, 600, 2], P('track', 'ifg'), may hold values from 0 to 249, as said below
- date_map: int32 [4, 250], replicated, may hold values from 0 to 319, as said below
- knots: int32 [32], replicated, may hold values from 0 to 319, as said below
- look: float32 [4, 3, 262144], P(None, None, 'pix'), may hold values from -1 to 1
Outputs:
- enu: float32 [3, 320, 262144], P(None, None, ('pix', 'ifg', 'track'))
- spline: float32 [3, 32, 262144], P(None, None, ('pix', 'ifg', 'track'))
The draws below stay inside these ranges and needn't reach their ends.
Inputs may be any that keep to these rules, and one draw needn't show every extreme that they name: pairs[t, k, 0] < pairs[t, k, 1] <= pairs[t, k, 0] + 5. `date_map`: the dates of one track map to distinct epochs. `knots`: strictly increasing, the first 0 and the last 319.
All inputs are finite; a program needn't handle non-finite values.
Results may differ from the reference program's by a relative error of at most 0.0003.
Values may be sent and summed in bfloat16 or wider, within the bound.
A program may use at most 128 MiB of HBM per device.

```python
import jax
import jax.numpy as jnp
from jax import lax

NDATE = 250
IFGS = 600
EPOCHS = 320
KNOTS = 32
SPAN = 5
PIX_DEV = 16384
TRACKS = 4
PIXELS = 262144
N_TRACK = 4
N_IFG = 4


def draw_phases(key, part):
    key_common, key_noise = jax.random.split(key, 2)
    common = 2.0 * jax.random.normal(key_common, (TRACKS, IFGS, 1), jnp.float32)
    ramp = 1.0 + 2.0 * jnp.arange(PIXELS, dtype=jnp.float32)[None, None, :] / PIXELS
    noise = jax.random.normal(key_noise, (TRACKS, IFGS, PIXELS), jnp.float32)
    values = common * ramp + noise
    return values.astype(jnp.bfloat16)


def draw_pairs(key, part):
    key_first, key_step = jax.random.split(key)
    first = jax.random.randint(key_first, (TRACKS, IFGS), 0, NDATE - SPAN)
    step = jax.random.randint(key_step, (TRACKS, IFGS), 1, SPAN + 1)
    first = first.at[:, 0].set(0).at[:, IFGS - 1].set(NDATE - 1 - SPAN)
    step = step.at[:, IFGS - 1].set(SPAN)
    return jnp.stack([first, first + step], axis=-1).astype(jnp.int32)


def draw_date_map(key, part):
    scores = jax.random.randint(key, (TRACKS, EPOCHS), 0, 2 ** 20) * EPOCHS + jnp.arange(EPOCHS, dtype=jnp.int32)[None, :]
    index = jnp.arange(EPOCHS, dtype=jnp.int32)[None, :]
    scores = jnp.where((index == 0) | (index == EPOCHS - 1), 2 ** 30, scores)
    chosen = lax_top(scores, NDATE)
    return jnp.sort(chosen, axis=1).astype(jnp.int32)


def lax_top(scores, count):
    return jax.lax.top_k(scores, count)[1].astype(jnp.int32)


def draw_knots(key, part):
    scores = jax.random.randint(key, (EPOCHS - 2,), 0, 2 ** 20) * EPOCHS + jnp.arange(EPOCHS - 2, dtype=jnp.int32)
    inner = jnp.sort(lax_top(scores, KNOTS - 2)) + 1
    head = jnp.zeros((1,), jnp.int32)
    tail = jnp.full((1,), EPOCHS - 1, jnp.int32)
    return jnp.concatenate([head, inner.astype(jnp.int32), tail]).astype(jnp.int32)


def shard_levels(rng, dims, pieces, least, top_value):
    level, own = 1.0, jax.random.fold_in(rng, 6)
    for axis_at, shards_of in pieces:
        steps = jnp.exp(jax.random.uniform(jax.random.fold_in(own, axis_at), (shards_of,), jnp.float32, least / len(pieces), top_value / len(pieces)))
        level = level * jnp.repeat(steps, dims[axis_at] // shards_of).reshape([-1 if axis == axis_at else 1 for axis in range(len(dims))])
    return level


def setup_inputs(seed: int = 0) -> dict:
    arg_keys = jax.random.split(jax.random.key(seed), 6)
    return {
        "phases": draw_phases(jax.random.fold_in(arg_keys[5], 71), 0),
        "pairs": draw_pairs(jax.random.fold_in(arg_keys[5], 71), 0),
        "date_map": draw_date_map(jax.random.fold_in(arg_keys[5], 71), 0),
        "knots": draw_knots(jax.random.fold_in(arg_keys[5], 71), 0),
        "look": jnp.clip(jax.random.uniform(arg_keys[4], (TRACKS, 3, PIXELS), jnp.float32, -1.0, 1.0) * shard_levels(arg_keys[4], (TRACKS, 3, PIXELS), ((2, 16),), -0.4, 0.0), -1.0, 1.0),
    }


damping = 0.5
ridge = 0.1
HIGH = lax.Precision.HIGHEST

def incidence(pair_rows, ndate):
    dates = jnp.arange(ndate, dtype=jnp.int32)[:, None]
    later = (dates == pair_rows[None, :, 1]).astype(jnp.float32)
    earlier = (dates == pair_rows[None, :, 0]).astype(jnp.float32)
    return later - earlier

def inverse_normal(incid):
    ndate = incid.shape[0]
    normal = jnp.dot(incid, incid.T, precision=HIGH) + damping * jnp.eye(ndate, dtype=jnp.float32)
    factor = jnp.linalg.cholesky(normal)
    return jax.scipy.linalg.cho_solve((factor, True), jnp.eye(ndate, dtype=jnp.float32))

def hat_basis(knots, n_epochs):
    spots = knots.astype(jnp.float32)
    left = jnp.concatenate([spots[:1] - 1.0, spots[:-1]])
    right = jnp.concatenate([spots[1:], spots[-1:] + 1.0])
    epochs = jnp.arange(n_epochs, dtype=jnp.float32)[:, None]
    rise = (epochs - left) / (spots - left)
    fall = (right - epochs) / (right - spots)
    return jnp.maximum(0.0, jnp.minimum(rise, fall))

def geometry(series, date_map, look, knots, n_epochs):
    epochs = jnp.arange(n_epochs, dtype=jnp.int32)
    onehot = (date_map[:, None, :] == epochs[None, :, None]).astype(jnp.float32)
    seen = jnp.sum(onehot, axis=2)
    resampled = jnp.einsum('tcd,tdp->tcp', onehot, series, precision=HIGH)

    def entry(first, second):
        value = jnp.einsum('tc,tp->cp', seen, look[:, first] * look[:, second], precision=HIGH)
        if first == second:
            value = value + ridge
        return value
    a00, a01, a02 = (entry(0, 0), entry(0, 1), entry(0, 2))
    a11, a12, a22 = (entry(1, 1), entry(1, 2), entry(2, 2))
    b_all = [jnp.sum(look[:, i][:, None, :] * resampled, axis=0) for i in range(3)]
    c00 = a11 * a22 - a12 * a12
    c01 = a02 * a12 - a01 * a22
    c02 = a01 * a12 - a02 * a11
    c11 = a00 * a22 - a02 * a02
    c12 = a01 * a02 - a00 * a12
    c22 = a00 * a11 - a01 * a01
    det = a00 * c00 + a01 * c01 + a02 * c02
    east = (c00 * b_all[0] + c01 * b_all[1] + c02 * b_all[2]) / det
    north = (c01 * b_all[0] + c11 * b_all[1] + c12 * b_all[2]) / det
    upward = (c02 * b_all[0] + c12 * b_all[1] + c22 * b_all[2]) / det
    enu = jnp.stack([east, north, upward])
    basis = hat_basis(knots, n_epochs)
    gram = jnp.dot(basis.T, basis, precision=HIGH)
    factor = jnp.linalg.cholesky(gram)
    fitter = jax.scipy.linalg.cho_solve((factor, True), basis.T)
    spline = jnp.einsum('kc,icp->ikp', fitter, enu, precision=HIGH)
    return (enu, spline)

def reference(phases, pairs, date_map, knots, look):
    stacked = []
    for track in range(TRACKS):
        incid = incidence(pairs[track], NDATE)
        ninv = inverse_normal(incid)
        rhs = jnp.dot(incid.astype(jnp.bfloat16).astype(jnp.float32), phases[track].astype(jnp.float32), preferred_element_type=jnp.float32)
        series = jnp.dot(ninv, rhs, precision=HIGH)
        series = series - jnp.mean(series, axis=1, keepdims=True)
        stacked.append(series)
    series_all = jnp.stack(stacked)
    width = PIX_DEV // (N_IFG * N_TRACK)
    blocks = PIXELS // width
    series_blocks = jnp.transpose(series_all.reshape(TRACKS, NDATE, blocks, width), (2, 0, 1, 3))
    look_blocks = jnp.transpose(look.reshape(TRACKS, 3, blocks, width), (2, 0, 1, 3))

    def one_block(items):
        return geometry(items[0], date_map, items[1], knots, EPOCHS)
    enu_blocks, spline_blocks = lax.map(one_block, (series_blocks, look_blocks))
    enu = jnp.transpose(enu_blocks, (1, 2, 0, 3)).reshape(3, EPOCHS, PIXELS)
    spline = jnp.transpose(spline_blocks, (1, 2, 0, 3)).reshape(3, KNOTS, PIXELS)
    return (enu, spline)
```

```python
import functools

import jax
import jax.numpy as jnp
from jax import lax
from jax.experimental import pallas as pl
from jax.experimental.pallas import tpu as pltpu
from jax.sharding import PartitionSpec as P

EPOCHS = 320
MESH = pl.DeviceIdType.MESH
HIGH = lax.Precision.HIGHEST
F32 = jnp.float32
BF16 = jnp.bfloat16
damping = 0.5
ridge = 0.1
BAND = 8
PAIRS_OF = ((0, 0), (0, 1), (0, 2), (1, 1), (1, 2), (2, 2))


def dot(a, b, dims=((1,), (0,)), precision=None):
    return lax.dot_general(a, b, (dims, ((), ())), precision=precision, preferred_element_type=F32)


def iota(shape, dim):
    return lax.broadcasted_iota(jnp.int32, shape, dim)


def invert_small_blocks(blocks):
    rows, lanes = blocks.shape
    state = blocks.reshape(rows // BAND, BAND, lanes)
    sub = iota(state.shape, 1)
    lane = iota(state.shape, 2) % BAND
    for k in range(BAND):
        row = state[:, k : k + 1, :]
        col = state[:, :, k : k + 1]
        inv = 1.0 / row[:, :, k : k + 1]
        scaled = row * inv
        inner = state - col * scaled
        at_row = jnp.where(lane == k, jnp.broadcast_to(inv, state.shape), jnp.broadcast_to(scaled, state.shape))
        off_row = jnp.where(lane == k, -col * inv, inner)
        state = jnp.where(sub == k, at_row, off_row)
    return state.reshape(rows, lanes)


def invert_banded(matrix):
    n = matrix.shape[0]
    lanes = 128
    row, col = iota((n, n), 0), iota((n, n), 1)
    block_row, block_col = row // BAND, col // BAND
    eye = (row == col).astype(F32)
    fold = (iota((n, lanes), 0) % BAND == iota((n, lanes), 1) % BAND).astype(F32)
    stride, inverse_diag, basis = 1, jnp.zeros((n, n), F32), eye
    while True:
        last = stride * BAND >= n
        if last:
            here_row = block_row == 0
            here_col = block_col == 0
        else:
            here_row = block_row % (2 * stride) == stride
            here_col = block_col % (2 * stride) == stride
        on_diag = here_row & here_col & (block_row == block_col)
        blocks = dot(jnp.where(on_diag, matrix, jnp.where(here_row, 0.0, eye)), fold, precision=HIGH)
        small = invert_small_blocks(blocks)
        small = jnp.concatenate([small] * (n // lanes), axis=1)
        level_inverse = jnp.where(on_diag, small, 0.0)
        inverse_diag = inverse_diag + level_inverse
        if last:
            break
        rest_row = block_row % (2 * stride) == 0
        rest_col = block_col % (2 * stride) == 0
        step = jnp.where(here_row & rest_col, dot(level_inverse, matrix, precision=HIGH), 0.0)
        matrix = jnp.where(rest_row & rest_col, matrix - dot(matrix, step, precision=HIGH), 0.0)
        basis = basis - dot(basis, step, precision=HIGH)
        stride *= 2
    scaled = dot(basis, inverse_diag, precision=HIGH)
    return dot(scaled, basis, ((1,), (1,)), precision=HIGH)


def parts(value, count):
    out = []
    for _ in range(count):
        piece = value.astype(BF16)
        out.append(piece)
        value = value - piece.astype(F32)
    return out


def spline_fitter(knots_row, n_epochs, n_knots):
    lane = iota(knots_row.shape, 1)
    before = pltpu.roll(knots_row, 1, 1)
    after = pltpu.roll(knots_row, knots_row.shape[1] - 1, 1)
    left = jnp.where(lane == 0, knots_row - 1.0, before)
    right = jnp.where(lane == n_knots - 1, knots_row + 1.0, after)
    valid = lane < n_knots
    up = jnp.where(valid, knots_row - left, 1.0)
    down = jnp.where(valid, right - knots_row, 1.0)
    epochs = iota((n_epochs, knots_row.shape[1]), 0).astype(F32)
    hat = jnp.maximum(0.0, jnp.minimum((epochs - left) / up, (right - epochs) / down))
    basis = jnp.where(valid, hat, 0.0)
    size = knots_row.shape[1]
    gram = dot(basis, basis, ((0,), (0,)), precision=HIGH)
    row, col = iota((size, size), 0), iota((size, size), 1)
    gram = jnp.where((row == col) & (row >= n_knots), 1.0, gram)
    inverse = invert_banded(gram)
    return dot(inverse[:n_knots], basis, ((1,), (1,)), precision=HIGH)


def target_of(me, k, n):
    if n != 4:
        return lax.rem(me + k + 1, n)
    half = jnp.minimum(me, 3 - me)
    near = (1 - half) if k == 0 else k + 1
    return jnp.where(me < 2, near, 3 - near)


def exchange_kernel(
    sizes, phases, pairs, date_map, knots, look,
    gathered, fit_hi, fit_lo, picks, table, look_out,
    pair_all, own, landed, weights, incid, series, sums, totals, look_rows,
    own_sem, pair_send, pair_recv, look_sem, sum_send, sum_recv, total_send, total_recv, z_send, z_recv, y_send, y_recv, y_own,
):
    n_track, n_ifg, n_pix, widths, n_dates, n_epochs, n_knots = sizes
    track, ifg, pix = lax.axis_index("track"), lax.axis_index("ifg"), lax.axis_index("pix")
    count, pixels = phases.shape[1], phases.shape[2]
    quarter = pixels // n_ifg
    final = quarter // n_track
    padded = 8 * -(-n_dates // 8)
    while padded & (padded - 1):
        padded += 8
    padded = max(padded, 128)

    ifg_target = [target_of(ifg, k, n_ifg) for k in range(n_ifg - 1)]
    track_target = [lax.rem(track + k + 1, n_track) for k in range(n_track - 1)]

    barrier = pltpu.get_barrier_semaphore()
    for k in range(n_ifg - 1):
        pl.semaphore_signal(barrier, inc=1, device_id={"ifg": ifg_target[k]}, device_id_type=MESH)
    for k in range(n_track - 1):
        pl.semaphore_signal(barrier, inc=1, device_id={"track": track_target[k]}, device_id_type=MESH)
    for k in range(1, n_pix):
        pl.semaphore_signal(barrier, inc=1, device_id={"pix": lax.rem(pix + k, n_pix)}, device_id_type=MESH)
    pl.semaphore_wait(barrier, n_ifg + n_track + n_pix - 3)

    own_copy = pltpu.make_async_copy(phases.at[0], own, own_sem)
    own_copy.start()
    pair_copies = []
    for k in range(n_ifg - 1):
        pair_copies.append(pltpu.make_async_remote_copy(
            src_ref=pairs.at[0], dst_ref=pair_all.at[ifg], send_sem=pair_send.at[k], recv_sem=pair_recv.at[ifg],
            device_id={"ifg": ifg_target[k]}, device_id_type=MESH))
        pair_copies[-1].start()
    pltpu.make_async_copy(pairs.at[0], pair_all.at[ifg], pair_recv.at[ifg]).start()
    look_at = pl.multiple_of(ifg * quarter + track * final, final)
    look_in = pltpu.make_async_copy(look.at[:, :, pl.ds(look_at, final)], look_rows, look_sem.at[0])
    look_in.start()
    z_waits = []
    at = 0
    for j, width in enumerate(widths):
        for k in range(n_ifg - 1):
            for part in range(n_track):
                start = pl.multiple_of(ifg_target[k] * quarter + part * final + at, 128)
                pltpu.make_async_remote_copy(
                    src_ref=phases.at[0, :, pl.ds(start, width)],
                    dst_ref=landed.at[ifg, :, pl.ds(n_track * at + part * width, width)],
                    send_sem=z_send.at[k, j], recv_sem=z_recv.at[ifg, j],
                    device_id={"ifg": ifg_target[k]}, device_id_type=MESH).start()
        for part in range(n_track):
            start = pl.multiple_of(ifg * quarter + part * final + at, 128)
            pltpu.make_async_copy(
                phases.at[0, :, pl.ds(start, width)],
                landed.at[ifg, :, pl.ds(n_track * at + part * width, width)],
                z_recv.at[ifg, j]).start()
        at += width

    own_copy.wait()
    piece = 1024 if pixels % 1024 == 0 else pixels
    ones = jnp.ones((8, piece), BF16)

    def add_piece(k, total):
        return total + dot(ones, own[:, pl.ds(pl.multiple_of(k * piece, piece), piece)], ((1,), (1,)))

    own_sum = lax.fori_loop(0, pixels // piece, add_piece, jnp.zeros((8, count), F32))
    sums[0] = own_sum[:1]

    knots_row = jnp.concatenate([knots[...], jnp.zeros((1, 128 - n_knots), jnp.int32)], axis=1).astype(F32)
    fitter = spline_fitter(knots_row, n_epochs, n_knots)
    fit_hi[...], fit_lo[...] = parts(fitter, 2)

    sum_copies = []
    for k in range(1, n_pix):
        sum_copies.append(pltpu.make_async_remote_copy(
            src_ref=sums.at[0], dst_ref=sums.at[k], send_sem=sum_send.at[k], recv_sem=sum_recv.at[k],
            device_id={"pix": lax.rem(pix + k, n_pix)}, device_id_type=MESH))
        sum_copies[-1].start()

    code = jnp.zeros((n_epochs, 1), jnp.int32)
    for t in range(n_track):
        hit = (iota((n_epochs, n_dates), 0) == date_map[t : t + 1, :]).astype(F32)
        code = code + (jnp.max(hit, axis=1, keepdims=True) > 0.5).astype(jnp.int32) * (1 << t)
    n_masks = 1 << n_track
    lane = iota((n_epochs, 3 * n_masks), 1)
    picks[...] = (lane % n_masks == code).astype(F32).astype(BF16)

    look_in.wait()
    look_out[...] = look_rows[...]
    mask = iota((n_masks, final), 0)
    bits = [((mask >> t) & 1).astype(F32) for t in range(n_track)]

    def entry(i, j):
        value = ridge if i == j else 0.0
        for t in range(n_track):
            value = value + bits[t] * (look_rows[i, t : t + 1, :] * look_rows[j, t : t + 1, :])
        return value

    a00, a01, a02, a11, a12, a22 = [entry(i, j) for i, j in PAIRS_OF]
    c00 = a11 * a22 - a12 * a12
    c01 = a02 * a12 - a01 * a22
    c02 = a01 * a12 - a02 * a11
    c11 = a00 * a22 - a02 * a02
    c12 = a01 * a02 - a00 * a12
    c22 = a00 * a11 - a01 * a01
    det = a00 * c00 + a01 * c01 + a02 * c02
    for e, cofactor in enumerate((c00, c01, c02, c11, c12, c22)):
        table[e] = jnp.concatenate(parts(cofactor / det, 3), axis=0)

    for s in range(n_ifg):
        pltpu.make_async_copy(pair_all.at[s], pair_all.at[s], pair_recv.at[s]).wait()
    normal = jnp.zeros((padded, padded), F32)
    dates = iota((padded, count), 0)
    for s in range(n_ifg):
        rows = pair_all[s]
        matrix = (dates == rows[1:2, :]).astype(F32) - (dates == rows[0:1, :]).astype(F32)
        incid[s] = matrix
        matrix = matrix.astype(BF16)
        normal = normal + dot(matrix, matrix, ((1,), (1,)))
    normal = normal + jnp.where(iota(normal.shape, 0) == iota(normal.shape, 1), damping, 0.0)
    inverse = invert_banded(normal)

    total = sums[0]
    for k in range(1, n_pix):
        pltpu.make_async_copy(sums.at[k], sums.at[k], sum_recv.at[k]).wait()
        total = total + sums[k]
    totals[ifg] = total

    my_map = date_map[pl.ds(track, 1), :]
    placed = (iota((n_epochs, n_dates), 0) == my_map).astype(F32)
    placed = dot(placed, inverse[:n_dates], precision=HIGH)
    for s in range(n_ifg):
        weight = dot(placed, incid[s], precision=HIGH)
        weights[s, 0], weights[s, 1] = parts(weight, 2)
    total_copies = []
    for k in range(n_ifg - 1):
        total_copies.append(pltpu.make_async_remote_copy(
            src_ref=totals.at[ifg], dst_ref=totals.at[ifg], send_sem=total_send.at[k], recv_sem=total_recv.at[ifg],
            device_id={"ifg": ifg_target[k]}, device_id_type=MESH))
        total_copies[-1].start()
    for k in range(n_ifg - 1):
        s = ifg_target[k]
        pltpu.make_async_copy(totals.at[s], totals.at[s], total_recv.at[s]).wait()
    mean = jnp.zeros((n_epochs, 1), F32)
    for s in range(n_ifg):
        weight = weights[s, 0].astype(F32) + weights[s, 1].astype(F32)
        mean = mean + jnp.sum(weight * totals[s], axis=1, keepdims=True)
    mean = mean / (pixels * n_pix)

    at = 0
    for j, width in enumerate(widths):
        for s in range(n_ifg):
            chunk = landed.at[s, :, pl.ds(n_track * at, n_track * width)]
            pltpu.make_async_copy(chunk, chunk, z_recv.at[s, j]).wait()
        for k in range(n_track):
            part = track_target[k] if k < n_track - 1 else track
            where = pl.multiple_of(n_track * at + part * width, 128)
            value = jnp.zeros((n_epochs, width), F32)
            for s in range(n_ifg):
                phase = landed[s, :, pl.ds(where, width)]
                value = value + dot(weights[s, 0], phase) + dot(weights[s, 1], phase)
            series[:, pl.ds(where, width)] = value - mean
            if k < n_track - 1:
                pltpu.make_async_remote_copy(
                    src_ref=series.at[:, pl.ds(where, width)], dst_ref=gathered.at[track, :, pl.ds(at, width)],
                    send_sem=y_send.at[k, j], recv_sem=y_recv.at[track, j],
                    device_id={"track": part}, device_id_type=MESH).start()
            else:
                pltpu.make_async_copy(
                    series.at[:, pl.ds(where, width)], gathered.at[track, :, pl.ds(at, width)], y_recv.at[track, j]).start()
        at += width

    for copy in pair_copies + sum_copies + total_copies:
        copy.wait_send()
    at = 0
    for j, width in enumerate(widths):
        for k in range(n_ifg - 1):
            chunk = landed.at[0, :, pl.ds(n_track * at, n_track * width)]
            pltpu.make_async_copy(chunk, chunk, z_send.at[k, j]).wait()
        for t in range(n_track):
            here = gathered.at[t, :, pl.ds(at, width)]
            pltpu.make_async_copy(here, here, y_recv.at[t, j]).wait()
        for k in range(n_track - 1):
            here = series.at[:, pl.ds(0, width)]
            pltpu.make_async_copy(here, here, y_send.at[k, j]).wait()
        at += width


def geometry_kernel(gathered, fit_hi, fit_lo, picks, table, look, enu, spline):
    n_track = gathered.shape[0]
    select = picks[...]
    entries = {}
    for e, (i, j) in enumerate(PAIRS_OF):
        entries[i, j] = entries[j, i] = dot(select, table[e])
    right = []
    for i in range(3):
        value = look[i, 0:1, :] * gathered[0]
        for t in range(1, n_track):
            value = value + look[i, t : t + 1, :] * gathered[t]
        right.append(value)
    for i in range(3):
        value = entries[i, 0] * right[0] + entries[i, 1] * right[1] + entries[i, 2] * right[2]
        enu[i] = value
        hi, lo = parts(value, 2)
        spline[i] = dot(fit_hi[...], hi) + dot(fit_hi[...], lo) + dot(fit_lo[...], hi)


def chunk_widths(final):
    if final == 1024:
        return (256, 256, 256, 128, 128)
    return (final // 2, final // 2) if final % 256 == 0 else (final,)


def shards(phases, pairs, date_map, knots, look):
    n_track, n_ifg, n_pix = lax.axis_size("track"), lax.axis_size("ifg"), lax.axis_size("pix")
    count, pixels = phases.shape[1], phases.shape[2]
    quarter = pixels // n_ifg
    final = quarter // n_track
    n_dates, n_epochs, n_knots = date_map.shape[1], EPOCHS, knots.shape[0]
    widths = chunk_widths(final)
    n = len(widths)
    padded = 128
    while padded < n_dates:
        padded *= 2
    n_masks = 1 << n_track
    sizes = (n_track, n_ifg, n_pix, widths, n_dates, n_epochs, n_knots)
    vmem = pl.BlockSpec(memory_space=pltpu.VMEM)
    anywhere = pl.BlockSpec(memory_space=pl.ANY)
    dma = pltpu.SemaphoreType.DMA
    gathered, fit_hi, fit_lo, picks, table, look_local = pl.pallas_call(
        functools.partial(exchange_kernel, sizes),
        out_shape=(
            jax.ShapeDtypeStruct((n_track, n_epochs, final), F32),
            jax.ShapeDtypeStruct((n_knots, n_epochs), BF16),
            jax.ShapeDtypeStruct((n_knots, n_epochs), BF16),
            jax.ShapeDtypeStruct((n_epochs, 3 * n_masks), BF16),
            jax.ShapeDtypeStruct((len(PAIRS_OF), 3 * n_masks, final), BF16),
            jax.ShapeDtypeStruct((3, n_track, final), F32),
        ),
        in_specs=[anywhere, anywhere, vmem, vmem, anywhere],
        out_specs=(anywhere, vmem, vmem, vmem, vmem, vmem),
        scratch_shapes=[
            pltpu.VMEM((n_ifg, 2, count), jnp.int32),
            pltpu.VMEM((count, pixels), BF16),
            pltpu.VMEM((n_ifg, count, quarter), BF16),
            pltpu.VMEM((n_ifg, 2, n_epochs, count), BF16),
            pltpu.VMEM((n_ifg, padded, count), F32),
            pltpu.VMEM((n_epochs, quarter), F32),
            pltpu.VMEM((n_pix, 1, count), F32),
            pltpu.VMEM((n_ifg, 1, count), F32),
            pltpu.VMEM((3, n_track, final), F32),
            dma(()), dma((n_ifg,)), dma((n_ifg,)), dma((1,)),
            dma((n_pix,)), dma((n_pix,)), dma((n_ifg,)), dma((n_ifg,)),
            dma((n_ifg, n)), dma((n_ifg, n)), dma((n_track, n)), dma((n_track, n)), dma(()),
        ],
        compiler_params=pltpu.CompilerParams(collective_id=0, has_side_effects=True, vmem_limit_bytes=56 << 20),
        name="exchange",
    )(phases, jnp.transpose(pairs, (0, 2, 1)), date_map, knots[None, :], jnp.transpose(look, (1, 0, 2)))
    width = min(final, 256)
    enu, spline = pl.pallas_call(
        geometry_kernel,
        grid=(final // width,),
        out_shape=(
            jax.ShapeDtypeStruct((3, n_epochs, final), F32),
            jax.ShapeDtypeStruct((3, n_knots, final), F32),
        ),
        in_specs=[
            pl.BlockSpec((n_track, n_epochs, width), lambda g: (0, 0, g)),
            pl.BlockSpec((n_knots, n_epochs), lambda g: (0, 0)),
            pl.BlockSpec((n_knots, n_epochs), lambda g: (0, 0)),
            pl.BlockSpec((n_epochs, 3 * n_masks), lambda g: (0, 0)),
            pl.BlockSpec((len(PAIRS_OF), 3 * n_masks, width), lambda g: (0, 0, g)),
            pl.BlockSpec((3, n_track, width), lambda g: (0, 0, g)),
        ],
        out_specs=(
            pl.BlockSpec((3, n_epochs, width), lambda g: (0, 0, g)),
            pl.BlockSpec((3, n_knots, width), lambda g: (0, 0, g)),
        ),
        compiler_params=pltpu.CompilerParams(vmem_limit_bytes=56 << 20),
        name="geometry",
    )(gathered, fit_hi, fit_lo, picks, table, look_local)
    return enu, spline


def solution(mesh):
    in_specs = (P("track", "ifg", "pix"), P("track", "ifg", None), P(), P(), P(None, None, "pix"))
    out_specs = (P(None, None, ("pix", "ifg", "track")), P(None, None, ("pix", "ifg", "track")))
    return jax.shard_map(shards, mesh=mesh, in_specs=in_specs, out_specs=out_specs, check_vma=False)
```

```python
import functools

import jax
import jax.numpy as jnp
from jax import lax
from jax.experimental import pallas as pl
from jax.experimental.pallas import tpu as pltpu
from jax.sharding import PartitionSpec as P

EPOCHS = 320
MESH = pl.DeviceIdType.MESH
HIGH = lax.Precision.HIGHEST
F32 = jnp.float32
BF16 = jnp.bfloat16
damping = 0.5
ridge = 0.1
BAND = 8
PAIRS_OF = ((0, 0), (0, 1), (0, 2), (1, 1), (1, 2), (2, 2))


def dot(a, b, dims=((1,), (0,)), precision=None):
    return lax.dot_general(a, b, (dims, ((), ())), precision=precision, preferred_element_type=F32)


def iota(shape, dim):
    return lax.broadcasted_iota(jnp.int32, shape, dim)


def invert_small_blocks(blocks):
    rows, lanes = blocks.shape
    state = blocks.reshape(rows // BAND, BAND, lanes)
    sub = iota(state.shape, 1)
    lane = iota(state.shape, 2) % BAND
    for k in range(BAND):
        row = state[:, k : k + 1, :]
        col = state[:, :, k : k + 1]
        inv = 1.0 / row[:, :, k : k + 1]
        scaled = row * inv
        inner = state - col * scaled
        at_row = jnp.where(lane == k, jnp.broadcast_to(inv, state.shape), jnp.broadcast_to(scaled, state.shape))
        off_row = jnp.where(lane == k, -col * inv, inner)
        state = jnp.where(sub == k, at_row, off_row)
    return state.reshape(rows, lanes)


def invert_banded(matrix):
    n = matrix.shape[0]
    lanes = 128
    row, col = iota((n, n), 0), iota((n, n), 1)
    block_row, block_col = row // BAND, col // BAND
    eye = (row == col).astype(F32)
    fold = (iota((n, lanes), 0) % BAND == iota((n, lanes), 1) % BAND).astype(F32)
    stride, inverse_diag, basis = 1, jnp.zeros((n, n), F32), eye
    while True:
        last = stride * BAND >= n
        if last:
            here_row = block_row == 0
            here_col = block_col == 0
        else:
            here_row = block_row % (2 * stride) == stride
            here_col = block_col % (2 * stride) == stride
        on_diag = here_row & here_col & (block_row == block_col)
        blocks = dot(jnp.where(on_diag, matrix, jnp.where(here_row, 0.0, eye)), fold, precision=HIGH)
        small = invert_small_blocks(blocks)
        small = jnp.concatenate([small] * (n // lanes), axis=1)
        level_inverse = jnp.where(on_diag, small, 0.0)
        inverse_diag = inverse_diag + level_inverse
        if last:
            break
        rest_row = block_row % (2 * stride) == 0
        rest_col = block_col % (2 * stride) == 0
        step = jnp.where(here_row & rest_col, dot(level_inverse, matrix, precision=HIGH), 0.0)
        matrix = jnp.where(rest_row & rest_col, matrix - dot(matrix, step, precision=HIGH), 0.0)
        basis = basis - dot(basis, step, precision=HIGH)
        stride *= 2
    scaled = dot(basis, inverse_diag, precision=HIGH)
    return dot(scaled, basis, ((1,), (1,)), precision=HIGH)


def parts(value, count):
    out = []
    for _ in range(count):
        piece = value.astype(BF16)
        out.append(piece)
        value = value - piece.astype(F32)
    return out


def spline_fitter(knots_row, n_epochs, n_knots):
    lane = iota(knots_row.shape, 1)
    before = pltpu.roll(knots_row, 1, 1)
    after = pltpu.roll(knots_row, knots_row.shape[1] - 1, 1)
    left = jnp.where(lane == 0, knots_row - 1.0, before)
    right = jnp.where(lane == n_knots - 1, knots_row + 1.0, after)
    valid = lane < n_knots
    up = jnp.where(valid, knots_row - left, 1.0)
    down = jnp.where(valid, right - knots_row, 1.0)
    epochs = iota((n_epochs, knots_row.shape[1]), 0).astype(F32)
    hat = jnp.maximum(0.0, jnp.minimum((epochs - left) / up, (right - epochs) / down))
    basis = jnp.where(valid, hat, 0.0)
    size = knots_row.shape[1]
    gram = dot(basis, basis, ((0,), (0,)), precision=HIGH)
    row, col = iota((size, size), 0), iota((size, size), 1)
    gram = jnp.where((row == col) & (row >= n_knots), 1.0, gram)
    inverse = invert_banded(gram)
    return dot(inverse[:n_knots], basis, ((1,), (1,)), precision=HIGH)


def target_of(me, k, n):
    if n != 4:
        return lax.rem(me + k + 1, n)
    half = jnp.minimum(me, 3 - me)
    near = (1 - half) if k == 0 else k + 1
    return jnp.where(me < 2, near, 3 - near)


def exchange_kernel(
    sizes, phases, pairs, date_map, knots, look,
    gathered, fit_hi, fit_lo, picks, table, look_out, mean_out,
    pair_all, own, landed, weights, incid, series, sums, totals, means, look_rows,
    own_sem, pair_send, pair_recv, look_sem, sum_send, sum_recv, total_send, total_recv, mean_send, mean_recv, z_send, z_recv, y_send, y_recv,
):
    n_track, n_ifg, n_pix, widths, n_dates, n_epochs, n_knots = sizes
    track, ifg, pix = lax.axis_index("track"), lax.axis_index("ifg"), lax.axis_index("pix")
    count, pixels = phases.shape[1], phases.shape[2]
    quarter = pixels // n_ifg
    final = quarter // n_track
    padded = 8 * -(-n_dates // 8)
    while padded & (padded - 1):
        padded += 8
    padded = max(padded, 128)

    ifg_target = [target_of(ifg, k, n_ifg) for k in range(n_ifg - 1)]
    track_target = [lax.rem(track + k + 1, n_track) for k in range(n_track - 1)]

    barrier = pltpu.get_barrier_semaphore()
    for k in range(n_ifg - 1):
        pl.semaphore_signal(barrier, inc=1, device_id={"ifg": ifg_target[k]}, device_id_type=MESH)
    for k in range(n_track - 1):
        pl.semaphore_signal(barrier, inc=1, device_id={"track": track_target[k]}, device_id_type=MESH)
    for k in range(1, n_pix):
        pl.semaphore_signal(barrier, inc=1, device_id={"pix": lax.rem(pix + k, n_pix)}, device_id_type=MESH)
    pl.semaphore_wait(barrier, n_ifg + n_track + n_pix - 3)

    own_copy = pltpu.make_async_copy(phases.at[0], own, own_sem)
    own_copy.start()
    pair_copies = []
    for k in range(n_ifg - 1):
        pair_copies.append(pltpu.make_async_remote_copy(
            src_ref=pairs.at[0], dst_ref=pair_all.at[ifg], send_sem=pair_send.at[k], recv_sem=pair_recv.at[ifg],
            device_id={"ifg": ifg_target[k]}, device_id_type=MESH))
        pair_copies[-1].start()
    pltpu.make_async_copy(pairs.at[0], pair_all.at[ifg], pair_recv.at[ifg]).start()
    look_at = pl.multiple_of(ifg * quarter + track * final, final)
    look_in = pltpu.make_async_copy(look.at[:, :, pl.ds(look_at, final)], look_rows, look_sem.at[0])
    look_in.start()
    starts = [sum(widths[:j]) for j in range(len(widths))]

    def send_chunk(j):
        at, width = starts[j], widths[j]
        for k in range(n_ifg - 1):
            for part in range(n_track):
                start = pl.multiple_of(ifg_target[k] * quarter + part * final + at, 128)
                pltpu.make_async_remote_copy(
                    src_ref=phases.at[0, :, pl.ds(start, width)],
                    dst_ref=landed.at[ifg, :, pl.ds(n_track * at + part * width, width)],
                    send_sem=z_send.at[k, j], recv_sem=z_recv.at[ifg, j],
                    device_id={"ifg": ifg_target[k]}, device_id_type=MESH).start()
        for part in range(n_track):
            start = pl.multiple_of(ifg * quarter + part * final + at, 128)
            pltpu.make_async_copy(
                phases.at[0, :, pl.ds(start, width)],
                landed.at[ifg, :, pl.ds(n_track * at + part * width, width)],
                z_recv.at[ifg, j]).start()

    batches = (1, min(3, len(widths)), len(widths))
    for j in range(batches[0]):
        send_chunk(j)

    own_copy.wait()
    piece = 1024 if pixels % 1024 == 0 else pixels
    ones = jnp.ones((8, piece), BF16)

    def add_piece(k, total):
        return total + dot(ones, own[:, pl.ds(pl.multiple_of(k * piece, piece), piece)], ((1,), (1,)))

    own_sum = lax.fori_loop(0, pixels // piece, add_piece, jnp.zeros((8, count), F32))
    sums[0] = own_sum[:1]

    code = jnp.zeros((n_epochs, 1), jnp.int32)
    for t in range(n_track):
        hit = (iota((n_epochs, n_dates), 0) == date_map[t : t + 1, :]).astype(F32)
        code = code + (jnp.max(hit, axis=1, keepdims=True) > 0.5).astype(jnp.int32) * (1 << t)
    n_masks = 1 << n_track
    lane = iota((n_epochs, 3 * n_masks), 1)
    picks[...] = (lane % n_masks == code).astype(F32).astype(BF16)

    sum_copies = []
    for k in range(1, n_pix):
        sum_copies.append(pltpu.make_async_remote_copy(
            src_ref=sums.at[0], dst_ref=sums.at[k], send_sem=sum_send.at[k], recv_sem=sum_recv.at[k],
            device_id={"pix": lax.rem(pix + k, n_pix)}, device_id_type=MESH))
        sum_copies[-1].start()
    for j in range(batches[0], batches[1]):
        send_chunk(j)

    knots_row = jnp.concatenate([knots[...], jnp.zeros((1, 128 - n_knots), jnp.int32)], axis=1).astype(F32)
    fitter = spline_fitter(knots_row, n_epochs, n_knots)
    fit_hi[...], fit_lo[...] = parts(fitter, 2)

    look_in.wait()
    look_out[...] = look_rows[...]
    mask = iota((n_masks, final), 0)
    bits = [((mask >> t) & 1).astype(F32) for t in range(n_track)]

    def entry(i, j):
        value = ridge if i == j else 0.0
        for t in range(n_track):
            value = value + bits[t] * (look_rows[i, t : t + 1, :] * look_rows[j, t : t + 1, :])
        return value

    a00, a01, a02, a11, a12, a22 = [entry(i, j) for i, j in PAIRS_OF]
    c00 = a11 * a22 - a12 * a12
    c01 = a02 * a12 - a01 * a22
    c02 = a01 * a12 - a02 * a11
    c11 = a00 * a22 - a02 * a02
    c12 = a01 * a02 - a00 * a12
    c22 = a00 * a11 - a01 * a01
    det = a00 * c00 + a01 * c01 + a02 * c02
    for e, cofactor in enumerate((c00, c01, c02, c11, c12, c22)):
        table[e] = jnp.concatenate(parts(cofactor / det, 3), axis=0)

    for s in range(n_ifg):
        pltpu.make_async_copy(pair_all.at[s], pair_all.at[s], pair_recv.at[s]).wait()
    normal = jnp.zeros((padded, padded), F32)
    dates = iota((padded, count), 0)
    for s in range(n_ifg):
        rows = pair_all[s]
        matrix = (dates == rows[1:2, :]).astype(F32) - (dates == rows[0:1, :]).astype(F32)
        incid[s] = matrix
        matrix = matrix.astype(BF16)
        normal = normal + dot(matrix, matrix, ((1,), (1,)))
    normal = normal + jnp.where(iota(normal.shape, 0) == iota(normal.shape, 1), damping, 0.0)
    inverse = invert_banded(normal)

    total = sums[0]
    for k in range(1, n_pix):
        pltpu.make_async_copy(sums.at[k], sums.at[k], sum_recv.at[k]).wait()
        total = total + sums[k]
    totals[ifg] = total

    my_map = date_map[pl.ds(track, 1), :]
    placed = (iota((n_epochs, n_dates), 0) == my_map).astype(F32)
    placed = dot(placed, inverse[:n_dates], precision=HIGH)
    for s in range(n_ifg):
        weight = dot(placed, incid[s], precision=HIGH)
        weights[s, 0], weights[s, 1] = parts(weight, 2)
    total_copies = []
    for k in range(n_ifg - 1):
        total_copies.append(pltpu.make_async_remote_copy(
            src_ref=totals.at[ifg], dst_ref=totals.at[ifg], send_sem=total_send.at[k], recv_sem=total_recv.at[ifg],
            device_id={"ifg": ifg_target[k]}, device_id_type=MESH))
        total_copies[-1].start()
    for j in range(batches[1], batches[2]):
        send_chunk(j)

    def send_mean():
        for k in range(n_ifg - 1):
            s = ifg_target[k]
            pltpu.make_async_copy(totals.at[s], totals.at[s], total_recv.at[s]).wait()
        mean = jnp.zeros((1, n_epochs), F32)
        for s in range(n_ifg):
            weight = weights[s, 0].astype(F32) + weights[s, 1].astype(F32)
            mean = mean + dot(totals[s], weight, ((1,), (1,)), precision=HIGH)
        means[track] = mean / (pixels * n_pix)
        for k in range(n_track - 1):
            mean_copies.append(pltpu.make_async_remote_copy(
                src_ref=means.at[track], dst_ref=means.at[track], send_sem=mean_send.at[k], recv_sem=mean_recv.at[track],
                device_id={"track": track_target[k]}, device_id_type=MESH))
            mean_copies[-1].start()

    mean_copies = []
    at = 0
    for j, width in enumerate(widths):
        if j == len(widths) - 1:
            send_mean()
        for s in range(n_ifg):
            chunk = landed.at[s, :, pl.ds(n_track * at, n_track * width)]
            pltpu.make_async_copy(chunk, chunk, z_recv.at[s, j]).wait()
        for k in range(n_track):
            part = track_target[k] if k < n_track - 1 else track
            where = pl.multiple_of(n_track * at + part * width, 128)
            value = jnp.zeros((n_epochs, width), F32)
            for s in range(n_ifg):
                phase = landed[s, :, pl.ds(where, width)]
                value = value + dot(weights[s, 0], phase) + dot(weights[s, 1], phase)
            series[:, pl.ds(where, width)] = value
            if k < n_track - 1:
                pltpu.make_async_remote_copy(
                    src_ref=series.at[:, pl.ds(where, width)], dst_ref=gathered.at[track, :, pl.ds(at, width)],
                    send_sem=y_send.at[k, j], recv_sem=y_recv.at[track, j],
                    device_id={"track": part}, device_id_type=MESH).start()
            else:
                pltpu.make_async_copy(
                    series.at[:, pl.ds(where, width)], gathered.at[track, :, pl.ds(at, width)], y_recv.at[track, j]).start()
        at += width

    for k in range(n_track - 1):
        t = track_target[k]
        pltpu.make_async_copy(means.at[t], means.at[t], mean_recv.at[t]).wait()
    eye = (iota((n_epochs, n_epochs), 0) == iota((n_epochs, n_epochs), 1)).astype(F32)
    mean_out[...] = jnp.concatenate(
        [dot(eye, means[t], ((1,), (1,)), precision=HIGH) for t in range(n_track)], axis=1)

    for copy in pair_copies + sum_copies + total_copies + mean_copies:
        copy.wait_send()
    at = 0
    for j, width in enumerate(widths):
        for k in range(n_ifg - 1):
            chunk = landed.at[0, :, pl.ds(n_track * at, n_track * width)]
            pltpu.make_async_copy(chunk, chunk, z_send.at[k, j]).wait()
        for t in range(n_track):
            here = gathered.at[t, :, pl.ds(at, width)]
            pltpu.make_async_copy(here, here, y_recv.at[t, j]).wait()
        for k in range(n_track - 1):
            here = series.at[:, pl.ds(0, width)]
            pltpu.make_async_copy(here, here, y_send.at[k, j]).wait()
        at += width


def geometry_kernel(gathered, fit_hi, fit_lo, picks, table, look, means, enu, spline):
    n_track = gathered.shape[0]
    select = picks[...]
    entries = {}
    for e, (i, j) in enumerate(PAIRS_OF):
        entries[i, j] = entries[j, i] = dot(select, table[e])
    tracks = [gathered[t] - means[:, t : t + 1] for t in range(n_track)]
    right = []
    for i in range(3):
        value = look[i, 0:1, :] * tracks[0]
        for t in range(1, n_track):
            value = value + look[i, t : t + 1, :] * tracks[t]
        right.append(value)
    for i in range(3):
        value = entries[i, 0] * right[0] + entries[i, 1] * right[1] + entries[i, 2] * right[2]
        enu[i] = value
        hi, lo = parts(value, 2)
        spline[i] = dot(fit_hi[...], hi) + dot(fit_hi[...], lo) + dot(fit_lo[...], hi)


def chunk_widths(final):
    if final == 1024:
        return (256, 256, 256, 128, 128)
    return (final // 2, final // 2) if final % 256 == 0 else (final,)


def shards(phases, pairs, date_map, knots, look):
    n_track, n_ifg, n_pix = lax.axis_size("track"), lax.axis_size("ifg"), lax.axis_size("pix")
    count, pixels = phases.shape[1], phases.shape[2]
    quarter = pixels // n_ifg
    final = quarter // n_track
    n_dates, n_epochs, n_knots = date_map.shape[1], EPOCHS, knots.shape[0]
    widths = chunk_widths(final)
    n = len(widths)
    padded = 128
    while padded < n_dates:
        padded *= 2
    n_masks = 1 << n_track
    sizes = (n_track, n_ifg, n_pix, widths, n_dates, n_epochs, n_knots)
    vmem = pl.BlockSpec(memory_space=pltpu.VMEM)
    anywhere = pl.BlockSpec(memory_space=pl.ANY)
    dma = pltpu.SemaphoreType.DMA
    gathered, fit_hi, fit_lo, picks, table, look_local, means = pl.pallas_call(
        functools.partial(exchange_kernel, sizes),
        out_shape=(
            jax.ShapeDtypeStruct((n_track, n_epochs, final), F32),
            jax.ShapeDtypeStruct((n_knots, n_epochs), BF16),
            jax.ShapeDtypeStruct((n_knots, n_epochs), BF16),
            jax.ShapeDtypeStruct((n_epochs, 3 * n_masks), BF16),
            jax.ShapeDtypeStruct((len(PAIRS_OF), 3 * n_masks, final), BF16),
            jax.ShapeDtypeStruct((3, n_track, final), F32),
            jax.ShapeDtypeStruct((n_epochs, n_track), F32),
        ),
        in_specs=[anywhere, anywhere, vmem, vmem, anywhere],
        out_specs=(anywhere,) + (vmem,) * 6,
        scratch_shapes=[
            pltpu.VMEM((n_ifg, 2, count), jnp.int32),
            pltpu.VMEM((count, pixels), BF16),
            pltpu.VMEM((n_ifg, count, quarter), BF16),
            pltpu.VMEM((n_ifg, 2, n_epochs, count), BF16),
            pltpu.VMEM((n_ifg, padded, count), F32),
            pltpu.VMEM((n_epochs, quarter), F32),
            pltpu.VMEM((n_pix, 1, count), F32),
            pltpu.VMEM((n_ifg, 1, count), F32),
            pltpu.VMEM((n_track, 1, n_epochs), F32),
            pltpu.VMEM((3, n_track, final), F32),
            dma(()), dma((n_ifg,)), dma((n_ifg,)), dma((1,)),
            dma((n_pix,)), dma((n_pix,)), dma((n_ifg,)), dma((n_ifg,)),
            dma((n_track,)), dma((n_track,)), dma((n_ifg, n)), dma((n_ifg, n)), dma((n_track, n)), dma((n_track, n)),
        ],
        compiler_params=pltpu.CompilerParams(collective_id=0, has_side_effects=True, vmem_limit_bytes=56 << 20),
        name="exchange",
    )(phases, jnp.transpose(pairs, (0, 2, 1)), date_map, knots[None, :], jnp.transpose(look, (1, 0, 2)))
    width = min(final, 256)
    enu, spline = pl.pallas_call(
        geometry_kernel,
        grid=(final // width,),
        out_shape=(
            jax.ShapeDtypeStruct((3, n_epochs, final), F32),
            jax.ShapeDtypeStruct((3, n_knots, final), F32),
        ),
        in_specs=[
            pl.BlockSpec((n_track, n_epochs, width), lambda g: (0, 0, g)),
            pl.BlockSpec((n_knots, n_epochs), lambda g: (0, 0)),
            pl.BlockSpec((n_knots, n_epochs), lambda g: (0, 0)),
            pl.BlockSpec((n_epochs, 3 * n_masks), lambda g: (0, 0)),
            pl.BlockSpec((len(PAIRS_OF), 3 * n_masks, width), lambda g: (0, 0, g)),
            pl.BlockSpec((3, n_track, width), lambda g: (0, 0, g)),
            pl.BlockSpec((n_epochs, n_track), lambda g: (0, 0)),
        ],
        out_specs=(
            pl.BlockSpec((3, n_epochs, width), lambda g: (0, 0, g)),
            pl.BlockSpec((3, n_knots, width), lambda g: (0, 0, g)),
        ),
        compiler_params=pltpu.CompilerParams(vmem_limit_bytes=56 << 20),
        name="geometry",
    )(gathered, fit_hi, fit_lo, picks, table, look_local, means)
    return enu, spline


def solution(mesh):
    in_specs = (P("track", "ifg", "pix"), P("track", "ifg", None), P(), P(), P(None, None, "pix"))
    out_specs = (P(None, None, ("pix", "ifg", "track")), P(None, None, ("pix", "ifg", "track")))
    return jax.shard_map(shards, mesh=mesh, in_specs=in_specs, out_specs=out_specs, check_vma=False)
```

```python
import functools

import jax
import jax.numpy as jnp
from jax import lax
from jax.experimental import pallas as pl
from jax.experimental.pallas import tpu as pltpu
from jax.sharding import PartitionSpec as P

EPOCHS = 320
MESH = pl.DeviceIdType.MESH
HIGH = lax.Precision.HIGHEST
F32 = jnp.float32
BF16 = jnp.bfloat16
damping = 0.5
ridge = 0.1
BAND = 8
PAIRS_OF = ((0, 0), (0, 1), (0, 2), (1, 1), (1, 2), (2, 2))


def dot(a, b, dims=((1,), (0,)), precision=None):
    return lax.dot_general(a, b, (dims, ((), ())), precision=precision, preferred_element_type=F32)


def iota(shape, dim):
    return lax.broadcasted_iota(jnp.int32, shape, dim)


def invert_small_blocks(blocks):
    rows, lanes = blocks.shape
    state = blocks.reshape(rows // BAND, BAND, lanes)
    sub = iota(state.shape, 1)
    lane = iota(state.shape, 2) % BAND
    for k in range(BAND):
        row = state[:, k : k + 1, :]
        col = state[:, :, k : k + 1]
        inv = 1.0 / row[:, :, k : k + 1]
        scaled = row * inv
        inner = state - col * scaled
        at_row = jnp.where(lane == k, jnp.broadcast_to(inv, state.shape), jnp.broadcast_to(scaled, state.shape))
        off_row = jnp.where(lane == k, -col * inv, inner)
        state = jnp.where(sub == k, at_row, off_row)
    return state.reshape(rows, lanes)


def invert_banded(matrix):
    n = matrix.shape[0]
    lanes = 128
    row, col = iota((n, n), 0), iota((n, n), 1)
    block_row, block_col = row // BAND, col // BAND
    eye = (row == col).astype(F32)
    fold = (iota((n, lanes), 0) % BAND == iota((n, lanes), 1) % BAND).astype(F32)
    stride, inverse_diag, basis = 1, jnp.zeros((n, n), F32), eye
    while True:
        last = stride * BAND >= n
        if last:
            here_row = block_row == 0
            here_col = block_col == 0
        else:
            here_row = block_row % (2 * stride) == stride
            here_col = block_col % (2 * stride) == stride
        on_diag = here_row & here_col & (block_row == block_col)
        blocks = dot(jnp.where(on_diag, matrix, jnp.where(here_row, 0.0, eye)), fold, precision=HIGH)
        small = invert_small_blocks(blocks)
        small = jnp.concatenate([small] * (n // lanes), axis=1)
        level_inverse = jnp.where(on_diag, small, 0.0)
        inverse_diag = inverse_diag + level_inverse
        if last:
            break
        rest_row = block_row % (2 * stride) == 0
        rest_col = block_col % (2 * stride) == 0
        step = jnp.where(here_row & rest_col, dot(level_inverse, matrix, precision=HIGH), 0.0)
        matrix = jnp.where(rest_row & rest_col, matrix - dot(matrix, step, precision=HIGH), 0.0)
        basis = basis - dot(basis, step, precision=HIGH)
        stride *= 2
    scaled = dot(basis, inverse_diag, precision=HIGH)
    return dot(scaled, basis, ((1,), (1,)), precision=HIGH)


def parts(value, count):
    out = []
    for _ in range(count):
        piece = value.astype(BF16)
        out.append(piece)
        value = value - piece.astype(F32)
    return out


def spline_fitter(knots_row, n_epochs, n_knots):
    lane = iota(knots_row.shape, 1)
    before = pltpu.roll(knots_row, 1, 1)
    after = pltpu.roll(knots_row, knots_row.shape[1] - 1, 1)
    left = jnp.where(lane == 0, knots_row - 1.0, before)
    right = jnp.where(lane == n_knots - 1, knots_row + 1.0, after)
    valid = lane < n_knots
    up = jnp.where(valid, knots_row - left, 1.0)
    down = jnp.where(valid, right - knots_row, 1.0)
    epochs = iota((n_epochs, knots_row.shape[1]), 0).astype(F32)
    hat = jnp.maximum(0.0, jnp.minimum((epochs - left) / up, (right - epochs) / down))
    basis = jnp.where(valid, hat, 0.0)
    size = knots_row.shape[1]
    gram = dot(basis, basis, ((0,), (0,)), precision=HIGH)
    row, col = iota((size, size), 0), iota((size, size), 1)
    gram = jnp.where((row == col) & (row >= n_knots), 1.0, gram)
    inverse = invert_banded(gram)
    return dot(inverse[:n_knots], basis, ((1,), (1,)), precision=HIGH)


def target_of(me, k, n):
    if n != 4:
        return lax.rem(me + k + 1, n)
    half = jnp.minimum(me, 3 - me)
    near = (1 - half) if k == 0 else k + 1
    return jnp.where(me < 2, near, 3 - near)


def exchange_kernel(
    sizes, phases, pairs, date_map, knots, look,
    gathered, fit, picks, table, look_out, mean_out,
    pair_all, own, landed, weights, incid, series, sums, totals, means, look_rows,
    own_sem, pair_send, pair_recv, look_sem, sum_send, sum_recv, total_send, total_recv, mean_send, mean_recv, z_send, z_recv, y_send, y_recv,
):
    n_track, n_ifg, n_pix, widths, n_dates, n_epochs, n_knots = sizes
    track, ifg, pix = lax.axis_index("track"), lax.axis_index("ifg"), lax.axis_index("pix")
    count, pixels = phases.shape[1], phases.shape[2]
    quarter = pixels // n_ifg
    final = quarter // n_track
    padded = 8 * -(-n_dates // 8)
    while padded & (padded - 1):
        padded += 8
    padded = max(padded, 128)

    ifg_target = [target_of(ifg, k, n_ifg) for k in range(n_ifg - 1)]
    steps = sorted(range(1, n_track), key=lambda k: -min(k, n_track - k))
    track_target = [lax.rem(track + k, n_track) for k in steps]
    parts_order = track_target + [track]

    barrier = pltpu.get_barrier_semaphore()
    for k in range(n_ifg - 1):
        pl.semaphore_signal(barrier, inc=1, device_id={"ifg": ifg_target[k]}, device_id_type=MESH)
    for k in range(n_track - 1):
        pl.semaphore_signal(barrier, inc=1, device_id={"track": track_target[k]}, device_id_type=MESH)
    for k in range(1, n_pix):
        pl.semaphore_signal(barrier, inc=1, device_id={"pix": lax.rem(pix + k, n_pix)}, device_id_type=MESH)
    pl.semaphore_wait(barrier, n_ifg + n_track + n_pix - 3)

    own_copy = pltpu.make_async_copy(phases.at[0], own, own_sem)
    own_copy.start()
    pair_copies = []
    for k in range(n_ifg - 1):
        pair_copies.append(pltpu.make_async_remote_copy(
            src_ref=pairs.at[0], dst_ref=pair_all.at[ifg], send_sem=pair_send.at[k], recv_sem=pair_recv.at[ifg],
            device_id={"ifg": ifg_target[k]}, device_id_type=MESH))
        pair_copies[-1].start()
    pltpu.make_async_copy(pairs.at[0], pair_all.at[ifg], pair_recv.at[ifg]).start()
    look_at = pl.multiple_of(ifg * quarter + track * final, final)
    look_in = pltpu.make_async_copy(look.at[:, :, pl.ds(look_at, final)], look_rows, look_sem.at[0])
    look_in.start()
    starts = [sum(widths[:j]) for j in range(len(widths))]

    def send_chunk(j):
        at, width = starts[j], widths[j]
        for k, part in enumerate(parts_order):
            here = pl.ds(n_track * at + k * width, width)
            for i in range(n_ifg - 1):
                start = pl.multiple_of(ifg_target[i] * quarter + part * final + at, 128)
                pltpu.make_async_remote_copy(
                    src_ref=phases.at[0, :, pl.ds(start, width)], dst_ref=landed.at[ifg, :, here],
                    send_sem=z_send.at[i, j, k], recv_sem=z_recv.at[ifg, j, k],
                    device_id={"ifg": ifg_target[i]}, device_id_type=MESH).start()
            start = pl.multiple_of(ifg * quarter + part * final + at, 128)
            pltpu.make_async_copy(
                phases.at[0, :, pl.ds(start, width)], landed.at[ifg, :, here], z_recv.at[ifg, j, k]).start()

    batches = (1, min(3, len(widths)), len(widths))
    for j in range(batches[0]):
        send_chunk(j)

    own_copy.wait()
    piece = 1024 if pixels % 1024 == 0 else pixels
    ones = jnp.ones((8, piece), BF16)

    def add_piece(k, total):
        return total + dot(ones, own[:, pl.ds(pl.multiple_of(k * piece, piece), piece)], ((1,), (1,)))

    own_sum = lax.fori_loop(0, pixels // piece, add_piece, jnp.zeros((8, count), F32))
    sums[0] = own_sum[:1]

    code = jnp.zeros((n_epochs, 1), jnp.int32)
    for t in range(n_track):
        hit = (iota((n_epochs, n_dates), 0) == date_map[t : t + 1, :]).astype(F32)
        code = code + (jnp.max(hit, axis=1, keepdims=True) > 0.5).astype(jnp.int32) * (1 << t)
    n_masks = 1 << n_track
    lane = iota((n_epochs, 3 * n_masks), 1)
    picks[...] = (lane % n_masks == code).astype(F32).astype(BF16)

    sum_copies = []
    for k in range(1, n_pix):
        sum_copies.append(pltpu.make_async_remote_copy(
            src_ref=sums.at[0], dst_ref=sums.at[k], send_sem=sum_send.at[k], recv_sem=sum_recv.at[k],
            device_id={"pix": lax.rem(pix + k, n_pix)}, device_id_type=MESH))
        sum_copies[-1].start()
    for j in range(batches[0], batches[1]):
        send_chunk(j)

    knots_row = jnp.concatenate([knots[...], jnp.zeros((1, 128 - n_knots), jnp.int32)], axis=1).astype(F32)
    fitter = spline_fitter(knots_row, n_epochs, n_knots)
    high, low = parts(fitter, 2)
    fit[...] = jnp.concatenate(
        [jnp.concatenate([high, high], axis=1), jnp.concatenate([low, jnp.zeros_like(low)], axis=1)], axis=0)

    look_in.wait()
    look_out[...] = look_rows[...]
    mask = iota((n_masks, final), 0)
    bits = [((mask >> t) & 1).astype(F32) for t in range(n_track)]

    def entry(i, j):
        value = ridge if i == j else 0.0
        for t in range(n_track):
            value = value + bits[t] * (look_rows[i, t : t + 1, :] * look_rows[j, t : t + 1, :])
        return value

    a00, a01, a02, a11, a12, a22 = [entry(i, j) for i, j in PAIRS_OF]
    c00 = a11 * a22 - a12 * a12
    c01 = a02 * a12 - a01 * a22
    c02 = a01 * a12 - a02 * a11
    c11 = a00 * a22 - a02 * a02
    c12 = a01 * a02 - a00 * a12
    c22 = a00 * a11 - a01 * a01
    det = a00 * c00 + a01 * c01 + a02 * c02
    for e, cofactor in enumerate((c00, c01, c02, c11, c12, c22)):
        table[e] = jnp.concatenate(parts(cofactor / det, 3), axis=0)

    for s in range(n_ifg):
        pltpu.make_async_copy(pair_all.at[s], pair_all.at[s], pair_recv.at[s]).wait()
    normal = jnp.zeros((padded, padded), F32)
    dates = iota((padded, count), 0)
    for s in range(n_ifg):
        rows = pair_all[s]
        matrix = (dates == rows[1:2, :]).astype(F32) - (dates == rows[0:1, :]).astype(F32)
        incid[s] = matrix
        matrix = matrix.astype(BF16)
        normal = normal + dot(matrix, matrix, ((1,), (1,)))
    normal = normal + jnp.where(iota(normal.shape, 0) == iota(normal.shape, 1), damping, 0.0)
    inverse = invert_banded(normal)

    total = sums[0]
    for k in range(1, n_pix):
        pltpu.make_async_copy(sums.at[k], sums.at[k], sum_recv.at[k]).wait()
        total = total + sums[k]
    totals[ifg] = total

    my_map = date_map[pl.ds(track, 1), :]
    placed = (iota((n_epochs, n_dates), 0) == my_map).astype(F32)
    placed = dot(placed, inverse[:n_dates], precision=HIGH)
    for s in range(n_ifg):
        weight = dot(placed, incid[s], precision=HIGH)
        weights[s, 0], weights[s, 1] = parts(weight, 2)
    total_copies = []
    for k in range(n_ifg - 1):
        total_copies.append(pltpu.make_async_remote_copy(
            src_ref=totals.at[ifg], dst_ref=totals.at[ifg], send_sem=total_send.at[k], recv_sem=total_recv.at[ifg],
            device_id={"ifg": ifg_target[k]}, device_id_type=MESH))
        total_copies[-1].start()
    for j in range(batches[1], batches[2]):
        send_chunk(j)

    def send_mean():
        for k in range(n_ifg - 1):
            s = ifg_target[k]
            pltpu.make_async_copy(totals.at[s], totals.at[s], total_recv.at[s]).wait()
        mean = jnp.zeros((1, n_epochs), F32)
        for s in range(n_ifg):
            weight = weights[s, 0].astype(F32) + weights[s, 1].astype(F32)
            mean = mean + dot(totals[s], weight, ((1,), (1,)), precision=HIGH)
        means[track] = mean / (pixels * n_pix)
        for k in range(n_track - 1):
            mean_copies.append(pltpu.make_async_remote_copy(
                src_ref=means.at[track], dst_ref=means.at[track], send_sem=mean_send.at[k], recv_sem=mean_recv.at[track],
                device_id={"track": track_target[k]}, device_id_type=MESH))
            mean_copies[-1].start()

    mean_copies = []
    at = 0
    for j, width in enumerate(widths):
        if j == len(widths) - 1:
            send_mean()
        for k, part in enumerate(parts_order):
            here = pl.ds(n_track * at + k * width, width)
            value = jnp.zeros((n_epochs, width), F32)
            for s in range(n_ifg):
                chunk = landed.at[s, :, here]
                pltpu.make_async_copy(chunk, chunk, z_recv.at[s, j, k]).wait()
            for s in range(n_ifg):
                phase = landed[s, :, here]
                value = value + dot(weights[s, 0], phase) + dot(weights[s, 1], phase)
            series[:, here] = value
            if k < n_track - 1:
                pltpu.make_async_remote_copy(
                    src_ref=series.at[:, here], dst_ref=gathered.at[track, :, pl.ds(at, width)],
                    send_sem=y_send.at[k, j], recv_sem=y_recv.at[track, j],
                    device_id={"track": part}, device_id_type=MESH).start()
            else:
                pltpu.make_async_copy(
                    series.at[:, here], gathered.at[track, :, pl.ds(at, width)], y_recv.at[track, j]).start()
        at += width

    for k in range(n_track - 1):
        t = track_target[k]
        pltpu.make_async_copy(means.at[t], means.at[t], mean_recv.at[t]).wait()
    eye = (iota((n_epochs, n_epochs), 0) == iota((n_epochs, n_epochs), 1)).astype(F32)
    mean_out[...] = jnp.concatenate(
        [dot(eye, means[t], ((1,), (1,)), precision=HIGH) for t in range(n_track)], axis=1)

    for copy in pair_copies + sum_copies + total_copies + mean_copies:
        copy.wait_send()
    at = 0
    for j, width in enumerate(widths):
        for i in range(n_ifg - 1):
            for k in range(n_track):
                chunk = landed.at[0, :, pl.ds(0, width)]
                pltpu.make_async_copy(chunk, chunk, z_send.at[i, j, k]).wait()
        for t in range(n_track):
            here = gathered.at[t, :, pl.ds(at, width)]
            pltpu.make_async_copy(here, here, y_recv.at[t, j]).wait()
        for k in range(n_track - 1):
            here = series.at[:, pl.ds(0, width)]
            pltpu.make_async_copy(here, here, y_send.at[k, j]).wait()
        at += width


def geometry_kernel(gathered, fit, picks, table, look, means, enu, spline):
    n_track = gathered.shape[0]
    select = picks[...]
    entries = {}
    for e, (i, j) in enumerate(PAIRS_OF):
        entries[i, j] = entries[j, i] = dot(select, table[e])
    tracks = [gathered[t] - means[:, t : t + 1] for t in range(n_track)]
    right = []
    for i in range(3):
        value = look[i, 0:1, :] * tracks[0]
        for t in range(1, n_track):
            value = value + look[i, t : t + 1, :] * tracks[t]
        right.append(value)
    for i in range(3):
        value = entries[i, 0] * right[0] + entries[i, 1] * right[1] + entries[i, 2] * right[2]
        enu[i] = value
        both = dot(fit[...], jnp.concatenate(parts(value, 2), axis=0))
        spline[i] = both[: both.shape[0] // 2] + both[both.shape[0] // 2 :]


def chunk_widths(final):
    if final == 1024:
        return (256, 256, 256, 128, 128)
    return (final // 2, final // 2) if final % 256 == 0 else (final,)


def shards(phases, pairs, date_map, knots, look):
    n_track, n_ifg, n_pix = lax.axis_size("track"), lax.axis_size("ifg"), lax.axis_size("pix")
    count, pixels = phases.shape[1], phases.shape[2]
    quarter = pixels // n_ifg
    final = quarter // n_track
    n_dates, n_epochs, n_knots = date_map.shape[1], EPOCHS, knots.shape[0]
    widths = chunk_widths(final)
    n = len(widths)
    padded = 128
    while padded < n_dates:
        padded *= 2
    n_masks = 1 << n_track
    sizes = (n_track, n_ifg, n_pix, widths, n_dates, n_epochs, n_knots)
    vmem = pl.BlockSpec(memory_space=pltpu.VMEM)
    anywhere = pl.BlockSpec(memory_space=pl.ANY)
    dma = pltpu.SemaphoreType.DMA
    gathered, fit, picks, table, look_local, means = pl.pallas_call(
        functools.partial(exchange_kernel, sizes),
        out_shape=(
            jax.ShapeDtypeStruct((n_track, n_epochs, final), F32),
            jax.ShapeDtypeStruct((2 * n_knots, 2 * n_epochs), BF16),
            jax.ShapeDtypeStruct((n_epochs, 3 * n_masks), BF16),
            jax.ShapeDtypeStruct((len(PAIRS_OF), 3 * n_masks, final), BF16),
            jax.ShapeDtypeStruct((3, n_track, final), F32),
            jax.ShapeDtypeStruct((n_epochs, n_track), F32),
        ),
        in_specs=[anywhere, anywhere, vmem, vmem, anywhere],
        out_specs=(anywhere,) + (vmem,) * 5,
        scratch_shapes=[
            pltpu.VMEM((n_ifg, 2, count), jnp.int32),
            pltpu.VMEM((count, pixels), BF16),
            pltpu.VMEM((n_ifg, count, quarter), BF16),
            pltpu.VMEM((n_ifg, 2, n_epochs, count), BF16),
            pltpu.VMEM((n_ifg, padded, count), F32),
            pltpu.VMEM((n_epochs, quarter), F32),
            pltpu.VMEM((n_pix, 1, count), F32),
            pltpu.VMEM((n_ifg, 1, count), F32),
            pltpu.VMEM((n_track, 1, n_epochs), F32),
            pltpu.VMEM((3, n_track, final), F32),
            dma(()), dma((n_ifg,)), dma((n_ifg,)), dma((1,)),
            dma((n_pix,)), dma((n_pix,)), dma((n_ifg,)), dma((n_ifg,)),
            dma((n_track,)), dma((n_track,)), dma((n_ifg, n, n_track)), dma((n_ifg, n, n_track)), dma((n_track, n)), dma((n_track, n)),
        ],
        compiler_params=pltpu.CompilerParams(collective_id=0, has_side_effects=True, vmem_limit_bytes=56 << 20),
        name="exchange",
    )(phases, jnp.transpose(pairs, (0, 2, 1)), date_map, knots[None, :], jnp.transpose(look, (1, 0, 2)))
    width = min(final, 256)
    enu, spline = pl.pallas_call(
        geometry_kernel,
        grid=(final // width,),
        out_shape=(
            jax.ShapeDtypeStruct((3, n_epochs, final), F32),
            jax.ShapeDtypeStruct((3, n_knots, final), F32),
        ),
        in_specs=[
            pl.BlockSpec((n_track, n_epochs, width), lambda g: (0, 0, g)),
            pl.BlockSpec((2 * n_knots, 2 * n_epochs), lambda g: (0, 0)),
            pl.BlockSpec((n_epochs, 3 * n_masks), lambda g: (0, 0)),
            pl.BlockSpec((len(PAIRS_OF), 3 * n_masks, width), lambda g: (0, 0, g)),
            pl.BlockSpec((3, n_track, width), lambda g: (0, 0, g)),
            pl.BlockSpec((n_epochs, n_track), lambda g: (0, 0)),
        ],
        out_specs=(
            pl.BlockSpec((3, n_epochs, width), lambda g: (0, 0, g)),
            pl.BlockSpec((3, n_knots, width), lambda g: (0, 0, g)),
        ),
        compiler_params=pltpu.CompilerParams(vmem_limit_bytes=56 << 20),
        name="geometry",
    )(gathered, fit, picks, table, look_local, means)
    return enu, spline


def solution(mesh):
    in_specs = (P("track", "ifg", "pix"), P("track", "ifg", None), P(), P(), P(None, None, "pix"))
    out_specs = (P(None, None, ("pix", "ifg", "track")), P(None, None, ("pix", "ifg", "track")))
    return jax.shard_map(shards, mesh=mesh, in_specs=in_specs, out_specs=out_specs, check_vma=False)
```

```python
import functools

import jax
import jax.numpy as jnp
from jax import lax
from jax.experimental import pallas as pl
from jax.experimental.pallas import tpu as pltpu
from jax.sharding import PartitionSpec as P

EPOCHS = 320
MESH = pl.DeviceIdType.MESH
HIGH = lax.Precision.HIGHEST
F32 = jnp.float32
BF16 = jnp.bfloat16
damping = 0.5
ridge = 0.1
BAND = 8
AHEAD_FIRST = 6
AHEAD = 3
MEAN_PIECE = 7
PAIRS_OF = ((0, 0), (0, 1), (0, 2), (1, 1), (1, 2), (2, 2))


def dot(a, b, dims=((1,), (0,)), precision=None):
    return lax.dot_general(a, b, (dims, ((), ())), precision=precision, preferred_element_type=F32)


def iota(shape, dim):
    return lax.broadcasted_iota(jnp.int32, shape, dim)


def invert_small_blocks(blocks):
    rows, lanes = blocks.shape
    state = blocks.reshape(rows // BAND, BAND, lanes)
    sub = iota(state.shape, 1)
    lane = iota(state.shape, 2) % BAND
    for k in range(BAND):
        row = state[:, k : k + 1, :]
        col = state[:, :, k : k + 1]
        inv = 1.0 / row[:, :, k : k + 1]
        scaled = row * inv
        inner = state - col * scaled
        at_row = jnp.where(lane == k, jnp.broadcast_to(inv, state.shape), jnp.broadcast_to(scaled, state.shape))
        off_row = jnp.where(lane == k, -col * inv, inner)
        state = jnp.where(sub == k, at_row, off_row)
    return state.reshape(rows, lanes)


def invert_banded(matrix):
    n = matrix.shape[0]
    lanes = 128
    row, col = iota((n, n), 0), iota((n, n), 1)
    block_row, block_col = row // BAND, col // BAND
    eye = (row == col).astype(F32)
    fold = (iota((n, lanes), 0) % BAND == iota((n, lanes), 1) % BAND).astype(F32)
    stride, inverse_diag, basis = 1, jnp.zeros((n, n), F32), eye
    while True:
        last = stride * BAND >= n
        if last:
            here_row = block_row == 0
            here_col = block_col == 0
        else:
            here_row = block_row % (2 * stride) == stride
            here_col = block_col % (2 * stride) == stride
        on_diag = here_row & here_col & (block_row == block_col)
        blocks = dot(jnp.where(on_diag, matrix, jnp.where(here_row, 0.0, eye)), fold, precision=HIGH)
        small = invert_small_blocks(blocks)
        small = jnp.concatenate([small] * (n // lanes), axis=1)
        level_inverse = jnp.where(on_diag, small, 0.0)
        inverse_diag = inverse_diag + level_inverse
        if last:
            break
        rest_row = block_row % (2 * stride) == 0
        rest_col = block_col % (2 * stride) == 0
        step = jnp.where(here_row & rest_col, dot(level_inverse, matrix, precision=HIGH), 0.0)
        matrix = jnp.where(rest_row & rest_col, matrix - dot(matrix, step, precision=HIGH), 0.0)
        basis = basis - dot(basis, step, precision=HIGH)
        stride *= 2
    scaled = dot(basis, inverse_diag, precision=HIGH)
    return dot(scaled, basis, ((1,), (1,)), precision=HIGH)


def parts(value, count):
    out = []
    for _ in range(count):
        piece = value.astype(BF16)
        out.append(piece)
        value = value - piece.astype(F32)
    return out


def spline_fitter(knots_row, n_epochs, n_knots):
    lane = iota(knots_row.shape, 1)
    before = pltpu.roll(knots_row, 1, 1)
    after = pltpu.roll(knots_row, knots_row.shape[1] - 1, 1)
    left = jnp.where(lane == 0, knots_row - 1.0, before)
    right = jnp.where(lane == n_knots - 1, knots_row + 1.0, after)
    valid = lane < n_knots
    up = jnp.where(valid, knots_row - left, 1.0)
    down = jnp.where(valid, right - knots_row, 1.0)
    epochs = iota((n_epochs, knots_row.shape[1]), 0).astype(F32)
    hat = jnp.maximum(0.0, jnp.minimum((epochs - left) / up, (right - epochs) / down))
    basis = jnp.where(valid, hat, 0.0)
    size = knots_row.shape[1]
    gram = dot(basis, basis, ((0,), (0,)), precision=HIGH)
    row, col = iota((size, size), 0), iota((size, size), 1)
    gram = jnp.where((row == col) & (row >= n_knots), 1.0, gram)
    inverse = invert_banded(gram)
    return dot(inverse[:n_knots], basis, ((1,), (1,)), precision=HIGH)


def target_of(me, k, n):
    if n != 4:
        return lax.rem(me + k + 1, n)
    half = jnp.minimum(me, 3 - me)
    near = (1 - half) if k == 0 else k + 1
    return jnp.where(me < 2, near, 3 - near)


def exchange_kernel(
    sizes, phases, pairs, date_map, knots, look,
    gathered, fit, picks, table, look_out, mean_out,
    pair_all, own, landed, weights, incid, series, sums, totals, means, look_rows,
    own_sem, pair_send, pair_recv, look_sem, sum_send, sum_recv, total_send, total_recv, mean_send, mean_recv, z_send, z_recv, y_send, y_recv,
):
    n_track, n_ifg, n_pix, widths, n_dates, n_epochs, n_knots = sizes
    ahead_first, ahead, mean_piece = AHEAD_FIRST, AHEAD, min(MEAN_PIECE, n_track * len(widths) - 5)
    track, ifg, pix = lax.axis_index("track"), lax.axis_index("ifg"), lax.axis_index("pix")
    count, pixels = phases.shape[1], phases.shape[2]
    quarter = pixels // n_ifg
    final = quarter // n_track
    padded = 8 * -(-n_dates // 8)
    while padded & (padded - 1):
        padded += 8
    padded = max(padded, 128)

    ifg_target = [target_of(ifg, k, n_ifg) for k in range(n_ifg - 1)]
    steps = sorted(range(1, n_track), key=lambda k: -min(k, n_track - k))
    track_target = [lax.rem(track + k, n_track) for k in steps]
    parts_order = track_target + [track]

    barrier = pltpu.get_barrier_semaphore()
    for k in range(n_ifg - 1):
        pl.semaphore_signal(barrier, inc=1, device_id={"ifg": ifg_target[k]}, device_id_type=MESH)
    for k in range(n_track - 1):
        pl.semaphore_signal(barrier, inc=1, device_id={"track": track_target[k]}, device_id_type=MESH)
    for k in range(1, n_pix):
        pl.semaphore_signal(barrier, inc=1, device_id={"pix": lax.rem(pix + k, n_pix)}, device_id_type=MESH)
    pl.semaphore_wait(barrier, n_ifg + n_track + n_pix - 3)

    own_copy = pltpu.make_async_copy(phases.at[0], own, own_sem)
    own_copy.start()
    pair_copies = []
    for k in range(n_ifg - 1):
        pair_copies.append(pltpu.make_async_remote_copy(
            src_ref=pairs.at[0], dst_ref=pair_all.at[ifg], send_sem=pair_send.at[k], recv_sem=pair_recv.at[ifg],
            device_id={"ifg": ifg_target[k]}, device_id_type=MESH))
        pair_copies[-1].start()
    pltpu.make_async_copy(pairs.at[0], pair_all.at[ifg], pair_recv.at[ifg]).start()
    look_at = pl.multiple_of(ifg * quarter + track * final, final)
    look_in = pltpu.make_async_copy(look.at[:, :, pl.ds(look_at, final)], look_rows, look_sem.at[0])
    look_in.start()
    starts = [sum(widths[:j]) for j in range(len(widths))]

    tail = max(len(widths) - 2, 0)
    order = [(j, k) for j in range(tail) for k in range(n_track)]
    order += [(j, k) for k in range(n_track) for j in range(tail, len(widths))]

    def send_piece(j, k):
        at, width, part = starts[j], widths[j], parts_order[k]
        here = pl.ds(n_track * at + k * width, width)
        for i in range(n_ifg - 1):
            start = pl.multiple_of(ifg_target[i] * quarter + part * final + at, 128)
            pltpu.make_async_remote_copy(
                src_ref=phases.at[0, :, pl.ds(start, width)], dst_ref=landed.at[ifg, :, here],
                send_sem=z_send.at[i, j, k], recv_sem=z_recv.at[ifg, j, k],
                device_id={"ifg": ifg_target[i]}, device_id_type=MESH).start()
        start = pl.multiple_of(ifg * quarter + part * final + at, 128)
        pltpu.make_async_copy(
            phases.at[0, :, pl.ds(start, width)], landed.at[ifg, :, here], z_recv.at[ifg, j, k]).start()

    ends = [sum(widths[j] for j, _ in order[: p + 1]) for p in range(len(order))]
    queued = [0]

    def send_upto(reach):
        while queued[0] < len(order) and ends[queued[0]] <= reach:
            send_piece(*order[queued[0]])
            queued[0] += 1

    send_upto(final)

    own_copy.wait()
    piece = 1024 if pixels % 1024 == 0 else pixels
    ones = jnp.ones((8, piece), BF16)

    def add_piece(k, total):
        return total + dot(ones, own[:, pl.ds(pl.multiple_of(k * piece, piece), piece)], ((1,), (1,)))

    own_sum = lax.fori_loop(0, pixels // piece, add_piece, jnp.zeros((8, count), F32))
    sums[0] = own_sum[:1]

    code = jnp.zeros((n_epochs, 1), jnp.int32)
    for t in range(n_track):
        hit = (iota((n_epochs, n_dates), 0) == date_map[t : t + 1, :]).astype(F32)
        code = code + (jnp.max(hit, axis=1, keepdims=True) > 0.5).astype(jnp.int32) * (1 << t)
    n_masks = 1 << n_track
    lane = iota((n_epochs, 3 * n_masks), 1)
    picks[...] = (lane % n_masks == code).astype(F32).astype(BF16)

    sum_copies = []
    for k in range(1, n_pix):
        sum_copies.append(pltpu.make_async_remote_copy(
            src_ref=sums.at[0], dst_ref=sums.at[k], send_sem=sum_send.at[k], recv_sem=sum_recv.at[k],
            device_id={"pix": lax.rem(pix + k, n_pix)}, device_id_type=MESH))
        sum_copies[-1].start()
    send_upto(ahead_first * final // 4)

    knots_row = jnp.concatenate([knots[...], jnp.zeros((1, 128 - n_knots), jnp.int32)], axis=1).astype(F32)
    fitter = spline_fitter(knots_row, n_epochs, n_knots)
    high, low = parts(fitter, 2)
    fit[...] = jnp.concatenate(
        [jnp.concatenate([high, high], axis=1), jnp.concatenate([low, jnp.zeros_like(low)], axis=1)], axis=0)

    look_in.wait()
    look_out[...] = look_rows[...]
    mask = iota((n_masks, final), 0)
    bits = [((mask >> t) & 1).astype(F32) for t in range(n_track)]

    def entry(i, j):
        value = ridge if i == j else 0.0
        for t in range(n_track):
            value = value + bits[t] * (look_rows[i, t : t + 1, :] * look_rows[j, t : t + 1, :])
        return value

    a00, a01, a02, a11, a12, a22 = [entry(i, j) for i, j in PAIRS_OF]
    c00 = a11 * a22 - a12 * a12
    c01 = a02 * a12 - a01 * a22
    c02 = a01 * a12 - a02 * a11
    c11 = a00 * a22 - a02 * a02
    c12 = a01 * a02 - a00 * a12
    c22 = a00 * a11 - a01 * a01
    det = a00 * c00 + a01 * c01 + a02 * c02
    for e, cofactor in enumerate((c00, c01, c02, c11, c12, c22)):
        table[e] = jnp.concatenate(parts(cofactor / det, 3), axis=0)

    for s in range(n_ifg):
        pltpu.make_async_copy(pair_all.at[s], pair_all.at[s], pair_recv.at[s]).wait()
    normal = jnp.zeros((padded, padded), F32)
    dates = iota((padded, count), 0)
    for s in range(n_ifg):
        rows = pair_all[s]
        matrix = (dates == rows[1:2, :]).astype(F32) - (dates == rows[0:1, :]).astype(F32)
        incid[s] = matrix
        matrix = matrix.astype(BF16)
        normal = normal + dot(matrix, matrix, ((1,), (1,)))
    normal = normal + jnp.where(iota(normal.shape, 0) == iota(normal.shape, 1), damping, 0.0)
    inverse = invert_banded(normal)

    total = sums[0]
    for k in range(1, n_pix):
        pltpu.make_async_copy(sums.at[k], sums.at[k], sum_recv.at[k]).wait()
        total = total + sums[k]
    totals[ifg] = total

    my_map = date_map[pl.ds(track, 1), :]
    placed = (iota((n_epochs, n_dates), 0) == my_map).astype(F32)
    placed = dot(placed, inverse[:n_dates], precision=HIGH)
    for s in range(n_ifg):
        weight = dot(placed, incid[s], precision=HIGH)
        weights[s, 0], weights[s, 1] = parts(weight, 2)
    total_copies = []
    for k in range(n_ifg - 1):
        total_copies.append(pltpu.make_async_remote_copy(
            src_ref=totals.at[ifg], dst_ref=totals.at[ifg], send_sem=total_send.at[k], recv_sem=total_recv.at[ifg],
            device_id={"ifg": ifg_target[k]}, device_id_type=MESH))
        total_copies[-1].start()

    def send_mean():
        for k in range(n_ifg - 1):
            s = ifg_target[k]
            pltpu.make_async_copy(totals.at[s], totals.at[s], total_recv.at[s]).wait()
        mean = jnp.zeros((1, n_epochs), F32)
        for s in range(n_ifg):
            weight = weights[s, 0].astype(F32) + weights[s, 1].astype(F32)
            mean = mean + dot(totals[s], weight, ((1,), (1,)), precision=HIGH)
        means[track] = mean / (pixels * n_pix)
        for k in range(n_track - 1):
            mean_copies.append(pltpu.make_async_remote_copy(
                src_ref=means.at[track], dst_ref=means.at[track], send_sem=mean_send.at[k], recv_sem=mean_recv.at[track],
                device_id={"track": track_target[k]}, device_id_type=MESH))
            mean_copies[-1].start()

    mean_copies = []
    def mean_columns():
        for k in range(n_track - 1):
            t = track_target[k]
            pltpu.make_async_copy(means.at[t], means.at[t], mean_recv.at[t]).wait()
        eye = (iota((n_epochs, n_epochs), 0) == iota((n_epochs, n_epochs), 1)).astype(F32)
        mean_out[...] = jnp.concatenate(
            [dot(eye, means[t], ((1,), (1,)), precision=HIGH) for t in range(n_track)], axis=1)

    for at_piece, (j, k) in enumerate(order):
        at, width, part = starts[j], widths[j], parts_order[k]
        if at_piece == mean_piece:
            send_mean()
        if at_piece == max(len(order) - 4, mean_piece + 1):
            mean_columns()
        here = pl.ds(n_track * at + k * width, width)
        for s in range(n_ifg):
            chunk = landed.at[s, :, here]
            pltpu.make_async_copy(chunk, chunk, z_recv.at[s, j, k]).wait()
        send_upto(n_track * final if at_piece == len(order) - 1 else ends[at_piece] + ahead * final // 4)
        value = jnp.zeros((n_epochs, width), F32)
        for s in range(n_ifg):
            phase = landed[s, :, here]
            value = value + dot(weights[s, 0], phase) + dot(weights[s, 1], phase)
        series[:, here] = value
        if k < n_track - 1:
            pltpu.make_async_remote_copy(
                src_ref=series.at[:, here], dst_ref=gathered.at[track, :, pl.ds(at, width)],
                send_sem=y_send.at[k, j], recv_sem=y_recv.at[track, j],
                device_id={"track": part}, device_id_type=MESH).start()
        else:
            pltpu.make_async_copy(
                series.at[:, here], gathered.at[track, :, pl.ds(at, width)], y_recv.at[track, j]).start()

    for copy in pair_copies + sum_copies + total_copies + mean_copies:
        copy.wait_send()
    at = 0
    for j, width in enumerate(widths):
        for i in range(n_ifg - 1):
            for k in range(n_track):
                chunk = landed.at[0, :, pl.ds(0, width)]
                pltpu.make_async_copy(chunk, chunk, z_send.at[i, j, k]).wait()
        for t in range(n_track):
            here = gathered.at[t, :, pl.ds(at, width)]
            pltpu.make_async_copy(here, here, y_recv.at[t, j]).wait()
        for k in range(n_track - 1):
            here = series.at[:, pl.ds(0, width)]
            pltpu.make_async_copy(here, here, y_send.at[k, j]).wait()
        at += width


def geometry_kernel(gathered, fit, picks, table, look, means, enu, spline):
    n_track = gathered.shape[0]
    select = picks[...]
    entries = {}
    for e, (i, j) in enumerate(PAIRS_OF):
        entries[i, j] = entries[j, i] = dot(select, table[e])
    tracks = [gathered[t] - means[:, t : t + 1] for t in range(n_track)]
    right = []
    for i in range(3):
        value = look[i, 0:1, :] * tracks[0]
        for t in range(1, n_track):
            value = value + look[i, t : t + 1, :] * tracks[t]
        right.append(value)
    for i in range(3):
        value = entries[i, 0] * right[0] + entries[i, 1] * right[1] + entries[i, 2] * right[2]
        enu[i] = value
        both = dot(fit[...], jnp.concatenate(parts(value, 2), axis=0))
        spline[i] = both[: both.shape[0] // 2] + both[both.shape[0] // 2 :]


def chunk_widths(final):
    if final == 1024:
        return (256, 256, 256, 128, 128)
    return (final // 2, final // 2) if final % 256 == 0 else (final,)


def shards(phases, pairs, date_map, knots, look):
    n_track, n_ifg, n_pix = lax.axis_size("track"), lax.axis_size("ifg"), lax.axis_size("pix")
    count, pixels = phases.shape[1], phases.shape[2]
    quarter = pixels // n_ifg
    final = quarter // n_track
    n_dates, n_epochs, n_knots = date_map.shape[1], EPOCHS, knots.shape[0]
    widths = chunk_widths(final)
    n = len(widths)
    padded = 128
    while padded < n_dates:
        padded *= 2
    n_masks = 1 << n_track
    sizes = (n_track, n_ifg, n_pix, widths, n_dates, n_epochs, n_knots)
    vmem = pl.BlockSpec(memory_space=pltpu.VMEM)
    anywhere = pl.BlockSpec(memory_space=pl.ANY)
    dma = pltpu.SemaphoreType.DMA
    gathered, fit, picks, table, look_local, means = pl.pallas_call(
        functools.partial(exchange_kernel, sizes),
        out_shape=(
            jax.ShapeDtypeStruct((n_track, n_epochs, final), F32),
            jax.ShapeDtypeStruct((2 * n_knots, 2 * n_epochs), BF16),
            jax.ShapeDtypeStruct((n_epochs, 3 * n_masks), BF16),
            jax.ShapeDtypeStruct((len(PAIRS_OF), 3 * n_masks, final), BF16),
            jax.ShapeDtypeStruct((3, n_track, final), F32),
            jax.ShapeDtypeStruct((n_epochs, n_track), F32),
        ),
        in_specs=[anywhere, anywhere, vmem, vmem, anywhere],
        out_specs=(anywhere,) + (vmem,) * 5,
        scratch_shapes=[
            pltpu.VMEM((n_ifg, 2, count), jnp.int32),
            pltpu.VMEM((count, pixels), BF16),
            pltpu.VMEM((n_ifg, count, quarter), BF16),
            pltpu.VMEM((n_ifg, 2, n_epochs, count), BF16),
            pltpu.VMEM((n_ifg, padded, count), F32),
            pltpu.VMEM((n_epochs, quarter), F32),
            pltpu.VMEM((n_pix, 1, count), F32),
            pltpu.VMEM((n_ifg, 1, count), F32),
            pltpu.VMEM((n_track, 1, n_epochs), F32),
            pltpu.VMEM((3, n_track, final), F32),
            dma(()), dma((n_ifg,)), dma((n_ifg,)), dma((1,)),
            dma((n_pix,)), dma((n_pix,)), dma((n_ifg,)), dma((n_ifg,)),
            dma((n_track,)), dma((n_track,)), dma((n_ifg, n, n_track)), dma((n_ifg, n, n_track)), dma((n_track, n)), dma((n_track, n)),
        ],
        compiler_params=pltpu.CompilerParams(collective_id=0, has_side_effects=True, vmem_limit_bytes=56 << 20),
        name="exchange",
    )(phases, jnp.transpose(pairs, (0, 2, 1)), date_map, knots[None, :], jnp.transpose(look, (1, 0, 2)))
    width = min(final, 256)
    enu, spline = pl.pallas_call(
        geometry_kernel,
        grid=(final // width,),
        out_shape=(
            jax.ShapeDtypeStruct((3, n_epochs, final), F32),
            jax.ShapeDtypeStruct((3, n_knots, final), F32),
        ),
        in_specs=[
            pl.BlockSpec((n_track, n_epochs, width), lambda g: (0, 0, g)),
            pl.BlockSpec((2 * n_knots, 2 * n_epochs), lambda g: (0, 0)),
            pl.BlockSpec((n_epochs, 3 * n_masks), lambda g: (0, 0)),
            pl.BlockSpec((len(PAIRS_OF), 3 * n_masks, width), lambda g: (0, 0, g)),
            pl.BlockSpec((3, n_track, width), lambda g: (0, 0, g)),
            pl.BlockSpec((n_epochs, n_track), lambda g: (0, 0)),
        ],
        out_specs=(
            pl.BlockSpec((3, n_epochs, width), lambda g: (0, 0, g)),
            pl.BlockSpec((3, n_knots, width), lambda g: (0, 0, g)),
        ),
        compiler_params=pltpu.CompilerParams(vmem_limit_bytes=56 << 20),
        name="geometry",
    )(gathered, fit, picks, table, look_local, means)
    return enu, spline


def solution(mesh):
    in_specs = (P("track", "ifg", "pix"), P("track", "ifg", None), P(), P(), P(None, None, "pix"))
    out_specs = (P(None, None, ("pix", "ifg", "track")), P(None, None, ("pix", "ifg", "track")))
    return jax.shard_map(shards, mesh=mesh, in_specs=in_specs, out_specs=out_specs, check_vma=False)
```

```python
import functools

import jax
import jax.numpy as jnp
from jax import lax
from jax.experimental import pallas as pl
from jax.experimental.pallas import tpu as pltpu
from jax.sharding import PartitionSpec as P

EPOCHS = 320
MESH = pl.DeviceIdType.MESH
HIGH = lax.Precision.HIGHEST
F32 = jnp.float32
BF16 = jnp.bfloat16
damping = 0.5
ridge = 0.1
BAND = 8
FIRST = 4
AHEAD_FIRST = 6
AHEAD = 3
MEAN_PIECE = 7
PAIRS_OF = ((0, 0), (0, 1), (0, 2), (1, 1), (1, 2), (2, 2))


def dot(a, b, dims=((1,), (0,)), precision=None):
    return lax.dot_general(a, b, (dims, ((), ())), precision=precision, preferred_element_type=F32)


def iota(shape, dim):
    return lax.broadcasted_iota(jnp.int32, shape, dim)


def invert_small_blocks(blocks):
    rows, lanes = blocks.shape
    state = blocks.reshape(rows // BAND, BAND, lanes)
    sub = iota(state.shape, 1)
    lane = iota(state.shape, 2) % BAND
    for k in range(BAND):
        row = state[:, k : k + 1, :]
        col = state[:, :, k : k + 1]
        inv = 1.0 / row[:, :, k : k + 1]
        scaled = row * inv
        inner = state - col * scaled
        at_row = jnp.where(lane == k, jnp.broadcast_to(inv, state.shape), jnp.broadcast_to(scaled, state.shape))
        off_row = jnp.where(lane == k, -col * inv, inner)
        state = jnp.where(sub == k, at_row, off_row)
    return state.reshape(rows, lanes)


def invert_banded(matrix):
    n = matrix.shape[0]
    lanes = 128
    row, col = iota((n, n), 0), iota((n, n), 1)
    block_row, block_col = row // BAND, col // BAND
    eye = (row == col).astype(F32)
    fold = (iota((n, lanes), 0) % BAND == iota((n, lanes), 1) % BAND).astype(F32)
    stride, inverse_diag, basis = 1, jnp.zeros((n, n), F32), eye
    while True:
        last = stride * BAND >= n
        if last:
            here_row = block_row == 0
            here_col = block_col == 0
        else:
            here_row = block_row % (2 * stride) == stride
            here_col = block_col % (2 * stride) == stride
        on_diag = here_row & here_col & (block_row == block_col)
        blocks = dot(jnp.where(on_diag, matrix, jnp.where(here_row, 0.0, eye)), fold, precision=HIGH)
        small = invert_small_blocks(blocks)
        small = jnp.concatenate([small] * (n // lanes), axis=1)
        level_inverse = jnp.where(on_diag, small, 0.0)
        inverse_diag = inverse_diag + level_inverse
        if last:
            break
        rest_row = block_row % (2 * stride) == 0
        rest_col = block_col % (2 * stride) == 0
        step = jnp.where(here_row & rest_col, dot(level_inverse, matrix, precision=HIGH), 0.0)
        matrix = jnp.where(rest_row & rest_col, matrix - dot(matrix, step, precision=HIGH), 0.0)
        basis = basis - dot(basis, step, precision=HIGH)
        stride *= 2
    scaled = dot(basis, inverse_diag, precision=HIGH)
    return dot(scaled, basis, ((1,), (1,)), precision=HIGH)


def parts(value, count):
    out = []
    for _ in range(count):
        piece = value.astype(BF16)
        out.append(piece)
        value = value - piece.astype(F32)
    return out


def spline_fitter(knots_row, n_epochs, n_knots):
    lane = iota(knots_row.shape, 1)
    before = pltpu.roll(knots_row, 1, 1)
    after = pltpu.roll(knots_row, knots_row.shape[1] - 1, 1)
    left = jnp.where(lane == 0, knots_row - 1.0, before)
    right = jnp.where(lane == n_knots - 1, knots_row + 1.0, after)
    valid = lane < n_knots
    up = jnp.where(valid, knots_row - left, 1.0)
    down = jnp.where(valid, right - knots_row, 1.0)
    epochs = iota((n_epochs, knots_row.shape[1]), 0).astype(F32)
    hat = jnp.maximum(0.0, jnp.minimum((epochs - left) / up, (right - epochs) / down))
    basis = jnp.where(valid, hat, 0.0)
    size = knots_row.shape[1]
    gram = dot(basis, basis, ((0,), (0,)), precision=HIGH)
    row, col = iota((size, size), 0), iota((size, size), 1)
    gram = jnp.where((row == col) & (row >= n_knots), 1.0, gram)
    inverse = invert_banded(gram)
    return dot(inverse[:n_knots], basis, ((1,), (1,)), precision=HIGH)


def target_of(me, k, n):
    if n != 4:
        return lax.rem(me + k + 1, n)
    half = jnp.minimum(me, 3 - me)
    near = (1 - half) if k == 0 else k + 1
    return jnp.where(me < 2, near, 3 - near)


def exchange_kernel(
    sizes, phases, pairs, date_map, knots, look,
    gathered, fit, picks, table, look_out, mean_out,
    pair_all, own, landed, weights, incid, series, sums, totals, means, look_rows,
    go, ready, own_sem, pair_send, pair_recv, look_sem, sum_send, sum_recv, total_send, total_recv, mean_send, mean_recv, z_send, z_recv, y_send, y_recv,
):
    n_track, n_ifg, n_pix, widths, n_dates, n_epochs, n_knots = sizes
    first, ahead_first, ahead, mean_piece = FIRST, AHEAD_FIRST, AHEAD, min(MEAN_PIECE, n_track * len(widths) - 5)
    track, ifg, pix = lax.axis_index("track"), lax.axis_index("ifg"), lax.axis_index("pix")
    count, pixels = phases.shape[1], phases.shape[2]
    quarter = pixels // n_ifg
    final = quarter // n_track
    padded = 8 * -(-n_dates // 8)
    while padded & (padded - 1):
        padded += 8
    padded = max(padded, 128)

    ifg_target = [target_of(ifg, k, n_ifg) for k in range(n_ifg - 1)]
    steps = sorted(range(1, n_track), key=lambda k: -min(k, n_track - k))
    track_target = [lax.rem(track + k, n_track) for k in steps]
    parts_order = track_target + [track]

    middle, helper = 1, 0
    others = [i for i in range(n_ifg) if i != middle]
    is_middle = ifg == middle
    barrier = pltpu.get_barrier_semaphore()

    @pl.when(is_middle)
    def _():
        pl.semaphore_wait(barrier, n_ifg - 1)
        for i in others:
            pl.semaphore_signal(go, inc=1, device_id={"ifg": i}, device_id_type=MESH)

    @pl.when(jnp.logical_not(is_middle))
    def _():
        pl.semaphore_signal(barrier, inc=1, device_id={"ifg": middle}, device_id_type=MESH)
        pl.semaphore_wait(go, 1)
        for k in range(n_track - 1):
            pl.semaphore_signal(barrier, inc=1, device_id={"track": track_target[k]}, device_id_type=MESH)
        for k in range(1, n_pix):
            pl.semaphore_signal(barrier, inc=1, device_id={"pix": lax.rem(pix + k, n_pix)}, device_id_type=MESH)

    def wait_for_peers():
        @pl.when(jnp.logical_not(is_middle))
        def _():
            pl.semaphore_wait(barrier, n_track + n_pix - 2)

        @pl.when(ifg == helper)
        def _():
            pl.semaphore_signal(ready, inc=1, device_id={"ifg": middle}, device_id_type=MESH)

        @pl.when(is_middle)
        def _():
            pl.semaphore_wait(ready, 1)

    own_copy = pltpu.make_async_copy(phases.at[0], own, own_sem)
    own_copy.start()
    pair_copies = []
    for k in range(n_ifg - 1):
        pair_copies.append(pltpu.make_async_remote_copy(
            src_ref=pairs.at[0], dst_ref=pair_all.at[ifg], send_sem=pair_send.at[k], recv_sem=pair_recv.at[ifg],
            device_id={"ifg": ifg_target[k]}, device_id_type=MESH))
        pair_copies[-1].start()
    pltpu.make_async_copy(pairs.at[0], pair_all.at[ifg], pair_recv.at[ifg]).start()
    look_at = pl.multiple_of(ifg * quarter + track * final, final)
    look_in = pltpu.make_async_copy(look.at[:, :, pl.ds(look_at, final)], look_rows, look_sem.at[0])
    look_in.start()
    starts = [sum(widths[:j]) for j in range(len(widths))]

    tail = max(len(widths) - 2, 0)
    order = [(j, k) for j in range(tail) for k in range(n_track)]
    order += [(j, k) for k in range(n_track) for j in range(tail, len(widths))]

    def send_piece(j, k):
        at, width, part = starts[j], widths[j], parts_order[k]
        here = pl.ds(n_track * at + k * width, width)
        for i in range(n_ifg - 1):
            start = pl.multiple_of(ifg_target[i] * quarter + part * final + at, 128)
            pltpu.make_async_remote_copy(
                src_ref=phases.at[0, :, pl.ds(start, width)], dst_ref=landed.at[ifg, :, here],
                send_sem=z_send.at[i, j, k], recv_sem=z_recv.at[ifg, j, k],
                device_id={"ifg": ifg_target[i]}, device_id_type=MESH).start()
        start = pl.multiple_of(ifg * quarter + part * final + at, 128)
        pltpu.make_async_copy(
            phases.at[0, :, pl.ds(start, width)], landed.at[ifg, :, here], z_recv.at[ifg, j, k]).start()

    ends = [sum(widths[j] for j, _ in order[: p + 1]) for p in range(len(order))]
    queued = [0]

    def send_upto(reach):
        while queued[0] < len(order) and ends[queued[0]] <= reach:
            send_piece(*order[queued[0]])
            queued[0] += 1

    send_upto(first * final // 4)

    own_copy.wait()
    piece = 1024 if pixels % 1024 == 0 else pixels
    ones = jnp.ones((8, piece), BF16)

    def add_piece(k, total):
        return total + dot(ones, own[:, pl.ds(pl.multiple_of(k * piece, piece), piece)], ((1,), (1,)))

    own_sum = lax.fori_loop(0, pixels // piece, add_piece, jnp.zeros((8, count), F32))
    sums[0] = own_sum[:1]

    code = jnp.zeros((n_epochs, 1), jnp.int32)
    for t in range(n_track):
        hit = (iota((n_epochs, n_dates), 0) == date_map[t : t + 1, :]).astype(F32)
        code = code + (jnp.max(hit, axis=1, keepdims=True) > 0.5).astype(jnp.int32) * (1 << t)
    n_masks = 1 << n_track
    lane = iota((n_epochs, 3 * n_masks), 1)
    picks[...] = (lane % n_masks == code).astype(F32).astype(BF16)

    knots_row = jnp.concatenate([knots[...], jnp.zeros((1, 128 - n_knots), jnp.int32)], axis=1).astype(F32)
    fitter = spline_fitter(knots_row, n_epochs, n_knots)
    high, low = parts(fitter, 2)
    fit[...] = jnp.concatenate(
        [jnp.concatenate([high, high], axis=1), jnp.concatenate([low, jnp.zeros_like(low)], axis=1)], axis=0)

    look_in.wait()
    look_out[...] = look_rows[...]
    mask = iota((n_masks, final), 0)
    bits = [((mask >> t) & 1).astype(F32) for t in range(n_track)]

    def entry(i, j):
        value = ridge if i == j else 0.0
        for t in range(n_track):
            value = value + bits[t] * (look_rows[i, t : t + 1, :] * look_rows[j, t : t + 1, :])
        return value

    a00, a01, a02, a11, a12, a22 = [entry(i, j) for i, j in PAIRS_OF]
    c00 = a11 * a22 - a12 * a12
    c01 = a02 * a12 - a01 * a22
    c02 = a01 * a12 - a02 * a11
    c11 = a00 * a22 - a02 * a02
    c12 = a01 * a02 - a00 * a12
    c22 = a00 * a11 - a01 * a01
    det = a00 * c00 + a01 * c01 + a02 * c02
    for e, cofactor in enumerate((c00, c01, c02, c11, c12, c22)):
        table[e] = jnp.concatenate(parts(cofactor / det, 3), axis=0)

    wait_for_peers()
    sum_copies = []
    for k in range(1, n_pix):
        sum_copies.append(pltpu.make_async_remote_copy(
            src_ref=sums.at[0], dst_ref=sums.at[k], send_sem=sum_send.at[k], recv_sem=sum_recv.at[k],
            device_id={"pix": lax.rem(pix + k, n_pix)}, device_id_type=MESH))
        sum_copies[-1].start()
    send_upto(ahead_first * final // 4)

    for s in range(n_ifg):
        pltpu.make_async_copy(pair_all.at[s], pair_all.at[s], pair_recv.at[s]).wait()
    normal = jnp.zeros((padded, padded), F32)
    dates = iota((padded, count), 0)
    for s in range(n_ifg):
        rows = pair_all[s]
        matrix = (dates == rows[1:2, :]).astype(F32) - (dates == rows[0:1, :]).astype(F32)
        incid[s] = matrix
        matrix = matrix.astype(BF16)
        normal = normal + dot(matrix, matrix, ((1,), (1,)))
    normal = normal + jnp.where(iota(normal.shape, 0) == iota(normal.shape, 1), damping, 0.0)
    inverse = invert_banded(normal)

    total = sums[0]
    for k in range(1, n_pix):
        pltpu.make_async_copy(sums.at[k], sums.at[k], sum_recv.at[k]).wait()
        total = total + sums[k]
    totals[ifg] = total

    my_map = date_map[pl.ds(track, 1), :]
    placed = (iota((n_epochs, n_dates), 0) == my_map).astype(F32)
    placed = dot(placed, inverse[:n_dates], precision=HIGH)
    for s in range(n_ifg):
        weight = dot(placed, incid[s], precision=HIGH)
        weights[s, 0], weights[s, 1] = parts(weight, 2)
    total_copies = []
    for k in range(n_ifg - 1):
        total_copies.append(pltpu.make_async_remote_copy(
            src_ref=totals.at[ifg], dst_ref=totals.at[ifg], send_sem=total_send.at[k], recv_sem=total_recv.at[ifg],
            device_id={"ifg": ifg_target[k]}, device_id_type=MESH))
        total_copies[-1].start()

    def send_mean():
        for k in range(n_ifg - 1):
            s = ifg_target[k]
            pltpu.make_async_copy(totals.at[s], totals.at[s], total_recv.at[s]).wait()
        mean = jnp.zeros((1, n_epochs), F32)
        for s in range(n_ifg):
            weight = weights[s, 0].astype(F32) + weights[s, 1].astype(F32)
            mean = mean + dot(totals[s], weight, ((1,), (1,)), precision=HIGH)
        means[track] = mean / (pixels * n_pix)
        for k in range(n_track - 1):
            mean_copies.append(pltpu.make_async_remote_copy(
                src_ref=means.at[track], dst_ref=means.at[track], send_sem=mean_send.at[k], recv_sem=mean_recv.at[track],
                device_id={"track": track_target[k]}, device_id_type=MESH))
            mean_copies[-1].start()

    mean_copies = []
    def mean_columns():
        for k in range(n_track - 1):
            t = track_target[k]
            pltpu.make_async_copy(means.at[t], means.at[t], mean_recv.at[t]).wait()
        eye = (iota((n_epochs, n_epochs), 0) == iota((n_epochs, n_epochs), 1)).astype(F32)
        mean_out[...] = jnp.concatenate(
            [dot(eye, means[t], ((1,), (1,)), precision=HIGH) for t in range(n_track)], axis=1)

    for at_piece, (j, k) in enumerate(order):
        at, width, part = starts[j], widths[j], parts_order[k]
        if at_piece == mean_piece:
            send_mean()
        if at_piece == max(len(order) - 4, mean_piece + 1):
            mean_columns()
        here = pl.ds(n_track * at + k * width, width)
        for s in range(n_ifg):
            chunk = landed.at[s, :, here]
            pltpu.make_async_copy(chunk, chunk, z_recv.at[s, j, k]).wait()
        send_upto(n_track * final if at_piece == len(order) - 1 else ends[at_piece] + ahead * final // 4)
        value = jnp.zeros((n_epochs, width), F32)
        for s in range(n_ifg):
            phase = landed[s, :, here]
            value = value + dot(weights[s, 0], phase) + dot(weights[s, 1], phase)
        series[:, here] = value
        if k < n_track - 1:
            pltpu.make_async_remote_copy(
                src_ref=series.at[:, here], dst_ref=gathered.at[track, :, pl.ds(at, width)],
                send_sem=y_send.at[k, j], recv_sem=y_recv.at[track, j],
                device_id={"track": part}, device_id_type=MESH).start()
        else:
            pltpu.make_async_copy(
                series.at[:, here], gathered.at[track, :, pl.ds(at, width)], y_recv.at[track, j]).start()

    for copy in pair_copies + sum_copies + total_copies + mean_copies:
        copy.wait_send()
    at = 0
    for j, width in enumerate(widths):
        for i in range(n_ifg - 1):
            for k in range(n_track):
                chunk = landed.at[0, :, pl.ds(0, width)]
                pltpu.make_async_copy(chunk, chunk, z_send.at[i, j, k]).wait()
        for t in range(n_track):
            here = gathered.at[t, :, pl.ds(at, width)]
            pltpu.make_async_copy(here, here, y_recv.at[t, j]).wait()
        for k in range(n_track - 1):
            here = series.at[:, pl.ds(0, width)]
            pltpu.make_async_copy(here, here, y_send.at[k, j]).wait()
        at += width


def geometry_kernel(gathered, fit, picks, table, look, means, enu, spline):
    n_track = gathered.shape[0]
    select = picks[...]
    entries = {}
    for e, (i, j) in enumerate(PAIRS_OF):
        entries[i, j] = entries[j, i] = dot(select, table[e])
    tracks = [gathered[t] - means[:, t : t + 1] for t in range(n_track)]
    right = []
    for i in range(3):
        value = look[i, 0:1, :] * tracks[0]
        for t in range(1, n_track):
            value = value + look[i, t : t + 1, :] * tracks[t]
        right.append(value)
    for i in range(3):
        value = entries[i, 0] * right[0] + entries[i, 1] * right[1] + entries[i, 2] * right[2]
        enu[i] = value
        both = dot(fit[...], jnp.concatenate(parts(value, 2), axis=0))
        spline[i] = both[: both.shape[0] // 2] + both[both.shape[0] // 2 :]


def chunk_widths(final):
    if final == 1024:
        return (256, 256, 256, 128, 128)
    return (final // 2, final // 2) if final % 256 == 0 else (final,)


def shards(phases, pairs, date_map, knots, look):
    n_track, n_ifg, n_pix = lax.axis_size("track"), lax.axis_size("ifg"), lax.axis_size("pix")
    count, pixels = phases.shape[1], phases.shape[2]
    quarter = pixels // n_ifg
    final = quarter // n_track
    n_dates, n_epochs, n_knots = date_map.shape[1], EPOCHS, knots.shape[0]
    widths = chunk_widths(final)
    n = len(widths)
    padded = 128
    while padded < n_dates:
        padded *= 2
    n_masks = 1 << n_track
    sizes = (n_track, n_ifg, n_pix, widths, n_dates, n_epochs, n_knots)
    vmem = pl.BlockSpec(memory_space=pltpu.VMEM)
    anywhere = pl.BlockSpec(memory_space=pl.ANY)
    dma = pltpu.SemaphoreType.DMA
    gathered, fit, picks, table, look_local, means = pl.pallas_call(
        functools.partial(exchange_kernel, sizes),
        out_shape=(
            jax.ShapeDtypeStruct((n_track, n_epochs, final), F32),
            jax.ShapeDtypeStruct((2 * n_knots, 2 * n_epochs), BF16),
            jax.ShapeDtypeStruct((n_epochs, 3 * n_masks), BF16),
            jax.ShapeDtypeStruct((len(PAIRS_OF), 3 * n_masks, final), BF16),
            jax.ShapeDtypeStruct((3, n_track, final), F32),
            jax.ShapeDtypeStruct((n_epochs, n_track), F32),
        ),
        in_specs=[anywhere, anywhere, vmem, vmem, anywhere],
        out_specs=(anywhere,) + (vmem,) * 5,
        scratch_shapes=[
            pltpu.VMEM((n_ifg, 2, count), jnp.int32),
            pltpu.VMEM((count, pixels), BF16),
            pltpu.VMEM((n_ifg, count, quarter), BF16),
            pltpu.VMEM((n_ifg, 2, n_epochs, count), BF16),
            pltpu.VMEM((n_ifg, padded, count), F32),
            pltpu.VMEM((n_epochs, quarter), F32),
            pltpu.VMEM((n_pix, 1, count), F32),
            pltpu.VMEM((n_ifg, 1, count), F32),
            pltpu.VMEM((n_track, 1, n_epochs), F32),
            pltpu.VMEM((3, n_track, final), F32),
            pltpu.SemaphoreType.REGULAR, pltpu.SemaphoreType.REGULAR,
            dma(()), dma((n_ifg,)), dma((n_ifg,)), dma((1,)),
            dma((n_pix,)), dma((n_pix,)), dma((n_ifg,)), dma((n_ifg,)),
            dma((n_track,)), dma((n_track,)), dma((n_ifg, n, n_track)), dma((n_ifg, n, n_track)), dma((n_track, n)), dma((n_track, n)),
        ],
        compiler_params=pltpu.CompilerParams(collective_id=0, has_side_effects=True, vmem_limit_bytes=56 << 20),
        name="exchange",
    )(phases, jnp.transpose(pairs, (0, 2, 1)), date_map, knots[None, :], jnp.transpose(look, (1, 0, 2)))
    width = min(final, 256)
    enu, spline = pl.pallas_call(
        geometry_kernel,
        grid=(final // width,),
        out_shape=(
            jax.ShapeDtypeStruct((3, n_epochs, final), F32),
            jax.ShapeDtypeStruct((3, n_knots, final), F32),
        ),
        in_specs=[
            pl.BlockSpec((n_track, n_epochs, width), lambda g: (0, 0, g)),
            pl.BlockSpec((2 * n_knots, 2 * n_epochs), lambda g: (0, 0)),
            pl.BlockSpec((n_epochs, 3 * n_masks), lambda g: (0, 0)),
            pl.BlockSpec((len(PAIRS_OF), 3 * n_masks, width), lambda g: (0, 0, g)),
            pl.BlockSpec((3, n_track, width), lambda g: (0, 0, g)),
            pl.BlockSpec((n_epochs, n_track), lambda g: (0, 0)),
        ],
        out_specs=(
            pl.BlockSpec((3, n_epochs, width), lambda g: (0, 0, g)),
            pl.BlockSpec((3, n_knots, width), lambda g: (0, 0, g)),
        ),
        compiler_params=pltpu.CompilerParams(vmem_limit_bytes=56 << 20),
        name="geometry",
    )(gathered, fit, picks, table, look_local, means)
    return enu, spline


def solution(mesh):
    in_specs = (P("track", "ifg", "pix"), P("track", "ifg", None), P(), P(), P(None, None, "pix"))
    out_specs = (P(None, None, ("pix", "ifg", "track")), P(None, None, ("pix", "ifg", "track")))
    return jax.shard_map(shards, mesh=mesh, in_specs=in_specs, out_specs=out_specs, check_vma=False)
```

```python
import functools

import jax
import jax.numpy as jnp
from jax import lax
from jax.experimental import pallas as pl
from jax.experimental.pallas import tpu as pltpu
from jax.sharding import PartitionSpec as P

EPOCHS = 320
MESH = pl.DeviceIdType.MESH
HIGH = lax.Precision.HIGHEST
F32 = jnp.float32
BF16 = jnp.bfloat16
damping = 0.5
ridge = 0.1
BAND = 8
FIRST = 4
AHEAD_FIRST = 6
AHEAD = 3
MEAN_PIECE = 7
PAIRS_OF = ((0, 0), (0, 1), (0, 2), (1, 1), (1, 2), (2, 2))


def dot(a, b, dims=((1,), (0,)), precision=None):
    return lax.dot_general(a, b, (dims, ((), ())), precision=precision, preferred_element_type=F32)


def iota(shape, dim):
    return lax.broadcasted_iota(jnp.int32, shape, dim)


def invert_small_blocks(blocks):
    rows, lanes = blocks.shape
    state = blocks.reshape(rows // BAND, BAND, lanes)
    sub = iota(state.shape, 1)
    lane = iota(state.shape, 2) % BAND
    for k in range(BAND):
        row = state[:, k : k + 1, :]
        col = state[:, :, k : k + 1]
        inv = 1.0 / row[:, :, k : k + 1]
        scaled = row * inv
        inner = state - col * scaled
        at_row = jnp.where(lane == k, jnp.broadcast_to(inv, state.shape), jnp.broadcast_to(scaled, state.shape))
        off_row = jnp.where(lane == k, -col * inv, inner)
        state = jnp.where(sub == k, at_row, off_row)
    return state.reshape(rows, lanes)


def invert_banded(matrix):
    n = matrix.shape[0]
    lanes = 128
    row, col = iota((n, n), 0), iota((n, n), 1)
    block_row, block_col = row // BAND, col // BAND
    eye = (row == col).astype(F32)
    fold = (iota((n, lanes), 0) % BAND == iota((n, lanes), 1) % BAND).astype(F32)
    stride, inverse_diag, basis = 1, jnp.zeros((n, n), F32), eye
    while True:
        last = stride * BAND >= n
        if last:
            here_row = block_row == 0
            here_col = block_col == 0
        else:
            here_row = block_row % (2 * stride) == stride
            here_col = block_col % (2 * stride) == stride
        on_diag = here_row & here_col & (block_row == block_col)
        blocks = dot(jnp.where(on_diag, matrix, jnp.where(here_row, 0.0, eye)), fold, precision=HIGH)
        small = invert_small_blocks(blocks)
        small = jnp.concatenate([small] * (n // lanes), axis=1)
        level_inverse = jnp.where(on_diag, small, 0.0)
        inverse_diag = inverse_diag + level_inverse
        if last:
            break
        rest_row = block_row % (2 * stride) == 0
        rest_col = block_col % (2 * stride) == 0
        step = jnp.where(here_row & rest_col, dot(level_inverse, matrix, precision=HIGH), 0.0)
        matrix = jnp.where(rest_row & rest_col, matrix - dot(matrix, step, precision=HIGH), 0.0)
        basis = basis - dot(basis, step, precision=HIGH)
        stride *= 2
    scaled = dot(basis, inverse_diag, precision=HIGH)
    return dot(scaled, basis, ((1,), (1,)), precision=HIGH)


def parts(value, count):
    out = []
    for _ in range(count):
        piece = value.astype(BF16)
        out.append(piece)
        value = value - piece.astype(F32)
    return out


def spline_fitter(knots_row, n_epochs, n_knots):
    lane = iota(knots_row.shape, 1)
    before = pltpu.roll(knots_row, 1, 1)
    after = pltpu.roll(knots_row, knots_row.shape[1] - 1, 1)
    left = jnp.where(lane == 0, knots_row - 1.0, before)
    right = jnp.where(lane == n_knots - 1, knots_row + 1.0, after)
    valid = lane < n_knots
    up = jnp.where(valid, knots_row - left, 1.0)
    down = jnp.where(valid, right - knots_row, 1.0)
    epochs = iota((n_epochs, knots_row.shape[1]), 0).astype(F32)
    hat = jnp.maximum(0.0, jnp.minimum((epochs - left) / up, (right - epochs) / down))
    basis = jnp.where(valid, hat, 0.0)
    size = knots_row.shape[1]
    gram = dot(basis, basis, ((0,), (0,)), precision=HIGH)
    row, col = iota((size, size), 0), iota((size, size), 1)
    gram = jnp.where((row == col) & (row >= n_knots), 1.0, gram)
    inverse = invert_banded(gram)
    return dot(inverse[:n_knots], basis, ((1,), (1,)), precision=HIGH)


def target_of(me, k, n):
    if n != 4:
        return lax.rem(me + k + 1, n)
    half = jnp.minimum(me, 3 - me)
    near = (1 - half) if k == 0 else k + 1
    return jnp.where(me < 2, near, 3 - near)


def exchange_kernel(
    sizes, phases, pairs, date_map, knots, look,
    gathered, fit, picks, table, look_out, mean_out,
    pair_all, own, landed, weights, incid, series, sums, totals, means, look_rows,
    go, ready, own_sem, pair_send, pair_recv, look_sem, sum_send, sum_recv, total_send, total_recv, mean_send, mean_recv, z_send, z_recv, y_send, y_recv,
):
    n_track, n_ifg, n_pix, widths, n_dates, n_epochs, n_knots = sizes
    first, ahead_first, ahead, mean_piece = FIRST, AHEAD_FIRST, AHEAD, min(MEAN_PIECE, n_track * len(widths) - 5)
    track, ifg, pix = lax.axis_index("track"), lax.axis_index("ifg"), lax.axis_index("pix")
    count, pixels = phases.shape[1], phases.shape[2]
    quarter = pixels // n_ifg
    final = quarter // n_track
    padded = 8 * -(-n_dates // 8)
    while padded & (padded - 1):
        padded += 8
    padded = max(padded, 128)

    ifg_target = [target_of(ifg, k, n_ifg) for k in range(n_ifg - 1)]
    steps = sorted(range(1, n_track), key=lambda k: -min(k, n_track - k))
    track_target = [lax.rem(track + k, n_track) for k in steps]
    parts_order = track_target + [track]

    middle, helper = 1, 0
    others = [i for i in range(n_ifg) if i != middle]
    is_middle = ifg == middle
    barrier = pltpu.get_barrier_semaphore()

    @pl.when(is_middle)
    def _():
        pl.semaphore_wait(barrier, n_ifg - 1)
        for i in others:
            pl.semaphore_signal(go, inc=1, device_id={"ifg": i}, device_id_type=MESH)

    @pl.when(jnp.logical_not(is_middle))
    def _():
        pl.semaphore_signal(barrier, inc=1, device_id={"ifg": middle}, device_id_type=MESH)
        pl.semaphore_wait(go, 1)
        for k in range(n_track - 1):
            pl.semaphore_signal(barrier, inc=1, device_id={"track": track_target[k]}, device_id_type=MESH)
        for k in range(1, n_pix):
            pl.semaphore_signal(barrier, inc=1, device_id={"pix": lax.rem(pix + k, n_pix)}, device_id_type=MESH)

    def wait_for_peers():
        @pl.when(jnp.logical_not(is_middle))
        def _():
            pl.semaphore_wait(barrier, n_track + n_pix - 2)

        @pl.when(ifg == helper)
        def _():
            pl.semaphore_signal(ready, inc=1, device_id={"ifg": middle}, device_id_type=MESH)

        @pl.when(is_middle)
        def _():
            pl.semaphore_wait(ready, 1)

    own_copy = pltpu.make_async_copy(phases.at[0], own, own_sem)
    own_copy.start()
    pair_copies = []
    for k in range(n_ifg - 1):
        pair_copies.append(pltpu.make_async_remote_copy(
            src_ref=pairs.at[0], dst_ref=pair_all.at[ifg], send_sem=pair_send.at[k], recv_sem=pair_recv.at[ifg],
            device_id={"ifg": ifg_target[k]}, device_id_type=MESH))
        pair_copies[-1].start()
    pltpu.make_async_copy(pairs.at[0], pair_all.at[ifg], pair_recv.at[ifg]).start()
    look_at = pl.multiple_of(ifg * quarter + track * final, final)
    look_in = pltpu.make_async_copy(look.at[:, :, pl.ds(look_at, final)], look_rows, look_sem.at[0])
    look_in.start()
    starts = [sum(widths[:j]) for j in range(len(widths))]

    tail = max(len(widths) - 2, 0)
    order = [(j, k) for j in range(tail) for k in range(n_track)]
    order += [(j, k) for k in range(n_track) for j in range(tail, len(widths))]

    def send_piece(j, k):
        at, width, part = starts[j], widths[j], parts_order[k]
        here = pl.ds(n_track * at + k * width, width)
        for i in range(n_ifg - 1):
            start = pl.multiple_of(ifg_target[i] * quarter + part * final + at, 128)
            pltpu.make_async_remote_copy(
                src_ref=phases.at[0, :, pl.ds(start, width)], dst_ref=landed.at[ifg, :, here],
                send_sem=z_send.at[i, j, k], recv_sem=z_recv.at[ifg, j, k],
                device_id={"ifg": ifg_target[i]}, device_id_type=MESH).start()
        start = pl.multiple_of(ifg * quarter + part * final + at, 128)
        pltpu.make_async_copy(
            phases.at[0, :, pl.ds(start, width)], landed.at[ifg, :, here], z_recv.at[ifg, j, k]).start()

    ends = [sum(widths[j] for j, _ in order[: p + 1]) for p in range(len(order))]
    queued = [0]

    def send_upto(reach):
        while queued[0] < len(order) and ends[queued[0]] <= reach:
            send_piece(*order[queued[0]])
            queued[0] += 1

    send_upto(first * final // 4)

    own_copy.wait()
    piece = 1024 if pixels % 1024 == 0 else pixels
    ones = jnp.ones((8, piece), BF16)

    def add_piece(k, total):
        return total + dot(ones, own[:, pl.ds(pl.multiple_of(k * piece, piece), piece)], ((1,), (1,)))

    own_sum = lax.fori_loop(0, pixels // piece, add_piece, jnp.zeros((8, count), F32))
    sums[0] = own_sum[:1]

    code = jnp.zeros((n_epochs, 1), jnp.int32)
    for t in range(n_track):
        hit = (iota((n_epochs, n_dates), 0) == date_map[t : t + 1, :]).astype(F32)
        code = code + (jnp.max(hit, axis=1, keepdims=True) > 0.5).astype(jnp.int32) * (1 << t)
    n_masks = 1 << n_track
    lane = iota((n_epochs, 3 * n_masks), 1)
    picks[...] = (lane % n_masks == code).astype(F32).astype(BF16)

    knots_row = jnp.concatenate([knots[...], jnp.zeros((1, 128 - n_knots), jnp.int32)], axis=1).astype(F32)
    fitter = spline_fitter(knots_row, n_epochs, n_knots)
    high, low = parts(fitter, 2)
    fit[...] = jnp.concatenate(
        [jnp.concatenate([high, high], axis=1), jnp.concatenate([low, jnp.zeros_like(low)], axis=1)], axis=0)

    look_in.wait()
    look_out[...] = look_rows[...]
    mask = iota((n_masks, final), 0)
    bits = [((mask >> t) & 1).astype(F32) for t in range(n_track)]

    def entry(i, j):
        value = ridge if i == j else 0.0
        for t in range(n_track):
            value = value + bits[t] * (look_rows[i, t : t + 1, :] * look_rows[j, t : t + 1, :])
        return value

    a00, a01, a02, a11, a12, a22 = [entry(i, j) for i, j in PAIRS_OF]
    c00 = a11 * a22 - a12 * a12
    c01 = a02 * a12 - a01 * a22
    c02 = a01 * a12 - a02 * a11
    c11 = a00 * a22 - a02 * a02
    c12 = a01 * a02 - a00 * a12
    c22 = a00 * a11 - a01 * a01
    det = a00 * c00 + a01 * c01 + a02 * c02
    for e, cofactor in enumerate((c00, c01, c02, c11, c12, c22)):
        table[e] = jnp.concatenate(parts(cofactor / det, 3), axis=0)

    wait_for_peers()
    sum_copies = []
    for k in range(1, n_pix):
        sum_copies.append(pltpu.make_async_remote_copy(
            src_ref=sums.at[0], dst_ref=sums.at[k], send_sem=sum_send.at[k], recv_sem=sum_recv.at[k],
            device_id={"pix": lax.rem(pix + k, n_pix)}, device_id_type=MESH))
        sum_copies[-1].start()
    send_upto(ahead_first * final // 4)

    for s in range(n_ifg):
        pltpu.make_async_copy(pair_all.at[s], pair_all.at[s], pair_recv.at[s]).wait()
    normal = jnp.zeros((padded, padded), F32)
    dates = iota((padded, count), 0)
    for s in range(n_ifg):
        rows = pair_all[s]
        matrix = (dates == rows[1:2, :]).astype(F32) - (dates == rows[0:1, :]).astype(F32)
        incid[s] = matrix
        matrix = matrix.astype(BF16)
        normal = normal + dot(matrix, matrix, ((1,), (1,)))
    normal = normal + jnp.where(iota(normal.shape, 0) == iota(normal.shape, 1), damping, 0.0)
    inverse = invert_banded(normal)

    total = sums[0]
    for k in range(1, n_pix):
        pltpu.make_async_copy(sums.at[k], sums.at[k], sum_recv.at[k]).wait()
        total = total + sums[k]
    totals[ifg] = total

    my_map = date_map[pl.ds(track, 1), :]
    placed = (iota((n_epochs, n_dates), 0) == my_map).astype(F32)
    placed = dot(placed, inverse[:n_dates], precision=HIGH)
    for s in range(n_ifg):
        weight = dot(placed, incid[s], precision=HIGH)
        weights[s, 0], weights[s, 1] = parts(weight, 2)
    total_copies = []
    for k in range(n_ifg - 1):
        total_copies.append(pltpu.make_async_remote_copy(
            src_ref=totals.at[ifg], dst_ref=totals.at[ifg], send_sem=total_send.at[k], recv_sem=total_recv.at[ifg],
            device_id={"ifg": ifg_target[k]}, device_id_type=MESH))
        total_copies[-1].start()

    def send_mean():
        for k in range(n_ifg - 1):
            s = ifg_target[k]
            pltpu.make_async_copy(totals.at[s], totals.at[s], total_recv.at[s]).wait()
        mean = jnp.zeros((1, n_epochs), F32)
        for s in range(n_ifg):
            weight = weights[s, 0].astype(F32) + weights[s, 1].astype(F32)
            mean = mean + dot(totals[s], weight, ((1,), (1,)), precision=HIGH)
        means[track] = mean / (pixels * n_pix)
        for k in range(n_track - 1):
            mean_copies.append(pltpu.make_async_remote_copy(
                src_ref=means.at[track], dst_ref=means.at[track], send_sem=mean_send.at[k], recv_sem=mean_recv.at[track],
                device_id={"track": track_target[k]}, device_id_type=MESH))
            mean_copies[-1].start()

    mean_copies = []
    def mean_columns():
        for k in range(n_track - 1):
            t = track_target[k]
            pltpu.make_async_copy(means.at[t], means.at[t], mean_recv.at[t]).wait()
        eye = (iota((n_epochs, n_epochs), 0) == iota((n_epochs, n_epochs), 1)).astype(F32)
        mean_out[...] = jnp.concatenate(
            [dot(eye, means[t], ((1,), (1,)), precision=HIGH) for t in range(n_track)], axis=1)

    for at_piece, (j, k) in enumerate(order):
        at, width, part = starts[j], widths[j], parts_order[k]
        if at_piece == mean_piece:
            send_mean()
        if at_piece == max(len(order) - 4, mean_piece + 1):
            mean_columns()
        here = pl.ds(n_track * at + k * width, width)
        for s in range(n_ifg):
            chunk = landed.at[s, :, here]
            pltpu.make_async_copy(chunk, chunk, z_recv.at[s, j, k]).wait()
        send_upto(n_track * final if at_piece == len(order) - 1 else ends[at_piece] + ahead * final // 4)
        value = jnp.zeros((n_epochs, width), F32)
        for s in range(n_ifg):
            phase = landed[s, :, here]
            value = value + dot(weights[s, 0], phase) + dot(weights[s, 1], phase)
        series[:, here] = value
        if k < n_track - 1:
            pltpu.make_async_remote_copy(
                src_ref=series.at[:, here], dst_ref=gathered.at[track, :, pl.ds(at, width)],
                send_sem=y_send.at[k, j], recv_sem=y_recv.at[track, j],
                device_id={"track": part}, device_id_type=MESH).start()
        else:
            pltpu.make_async_copy(
                series.at[:, here], gathered.at[track, :, pl.ds(at, width)], y_recv.at[track, j]).start()

    for copy in pair_copies + sum_copies + total_copies + mean_copies:
        copy.wait_send()
    at = 0
    for j, width in enumerate(widths):
        for i in range(n_ifg - 1):
            for k in range(n_track):
                chunk = landed.at[0, :, pl.ds(0, width)]
                pltpu.make_async_copy(chunk, chunk, z_send.at[i, j, k]).wait()
        for t in range(n_track):
            here = gathered.at[t, :, pl.ds(at, width)]
            pltpu.make_async_copy(here, here, y_recv.at[t, j]).wait()
        for k in range(n_track - 1):
            here = series.at[:, pl.ds(0, width)]
            pltpu.make_async_copy(here, here, y_send.at[k, j]).wait()
        at += width


def geometry_kernel(gathered, fit, picks, table, look, means, enu, spline):
    n_track = gathered.shape[0]
    select = picks[...]
    entries = {}
    for e, (i, j) in enumerate(PAIRS_OF):
        entries[i, j] = entries[j, i] = dot(select, table[e])
    tracks = [gathered[t] - means[:, t : t + 1] for t in range(n_track)]
    right = []
    for i in range(3):
        value = look[i, 0:1, :] * tracks[0]
        for t in range(1, n_track):
            value = value + look[i, t : t + 1, :] * tracks[t]
        right.append(value)
    for i in range(3):
        value = entries[i, 0] * right[0] + entries[i, 1] * right[1] + entries[i, 2] * right[2]
        enu[i] = value
        both = dot(fit[...], jnp.concatenate(parts(value, 2), axis=0))
        spline[i] = both[: both.shape[0] // 2] + both[both.shape[0] // 2 :]


def stay(value):
    return pltpu.with_memory_space_constraint(value, pltpu.HBM)


def chunk_widths(final):
    if final == 1024:
        return (256, 256, 256, 128, 128)
    return (final // 2, final // 2) if final % 256 == 0 else (final,)


def shards(phases, pairs, date_map, knots, look):
    n_track, n_ifg, n_pix = lax.axis_size("track"), lax.axis_size("ifg"), lax.axis_size("pix")
    count, pixels = phases.shape[1], phases.shape[2]
    quarter = pixels // n_ifg
    final = quarter // n_track
    n_dates, n_epochs, n_knots = date_map.shape[1], EPOCHS, knots.shape[0]
    widths = chunk_widths(final)
    n = len(widths)
    padded = 128
    while padded < n_dates:
        padded *= 2
    n_masks = 1 << n_track
    sizes = (n_track, n_ifg, n_pix, widths, n_dates, n_epochs, n_knots)
    vmem = pl.BlockSpec(memory_space=pltpu.VMEM)
    anywhere = pl.BlockSpec(memory_space=pl.ANY)
    outside = pl.BlockSpec(memory_space=pltpu.HBM)
    dma = pltpu.SemaphoreType.DMA
    gathered, fit, picks, table, look_local, means = pl.pallas_call(
        functools.partial(exchange_kernel, sizes),
        out_shape=(
            jax.ShapeDtypeStruct((n_track, n_epochs, final), F32),
            jax.ShapeDtypeStruct((2 * n_knots, 2 * n_epochs), BF16),
            jax.ShapeDtypeStruct((n_epochs, 3 * n_masks), BF16),
            jax.ShapeDtypeStruct((len(PAIRS_OF), 3 * n_masks, final), BF16),
            jax.ShapeDtypeStruct((3, n_track, final), F32),
            jax.ShapeDtypeStruct((n_epochs, n_track), F32),
        ),
        in_specs=[outside, outside, vmem, vmem, outside],
        out_specs=(anywhere,) + (vmem,) * 5,
        scratch_shapes=[
            pltpu.VMEM((n_ifg, 2, count), jnp.int32),
            pltpu.VMEM((count, pixels), BF16),
            pltpu.VMEM((n_ifg, count, quarter), BF16),
            pltpu.VMEM((n_ifg, 2, n_epochs, count), BF16),
            pltpu.VMEM((n_ifg, padded, count), F32),
            pltpu.VMEM((n_epochs, quarter), F32),
            pltpu.VMEM((n_pix, 1, count), F32),
            pltpu.VMEM((n_ifg, 1, count), F32),
            pltpu.VMEM((n_track, 1, n_epochs), F32),
            pltpu.VMEM((3, n_track, final), F32),
            pltpu.SemaphoreType.REGULAR, pltpu.SemaphoreType.REGULAR,
            dma(()), dma((n_ifg,)), dma((n_ifg,)), dma((1,)),
            dma((n_pix,)), dma((n_pix,)), dma((n_ifg,)), dma((n_ifg,)),
            dma((n_track,)), dma((n_track,)), dma((n_ifg, n, n_track)), dma((n_ifg, n, n_track)), dma((n_track, n)), dma((n_track, n)),
        ],
        compiler_params=pltpu.CompilerParams(collective_id=0, has_side_effects=True, vmem_limit_bytes=28 << 20),
        name="exchange",
    )(stay(phases), stay(jnp.transpose(pairs, (0, 2, 1))), stay(date_map), stay(knots[None, :]), stay(jnp.transpose(look, (1, 0, 2))))
    width = min(final, 256)
    enu, spline = pl.pallas_call(
        geometry_kernel,
        grid=(final // width,),
        out_shape=(
            jax.ShapeDtypeStruct((3, n_epochs, final), F32),
            jax.ShapeDtypeStruct((3, n_knots, final), F32),
        ),
        in_specs=[
            pl.BlockSpec((n_track, n_epochs, width), lambda g: (0, 0, g)),
            pl.BlockSpec((2 * n_knots, 2 * n_epochs), lambda g: (0, 0)),
            pl.BlockSpec((n_epochs, 3 * n_masks), lambda g: (0, 0)),
            pl.BlockSpec((len(PAIRS_OF), 3 * n_masks, width), lambda g: (0, 0, g)),
            pl.BlockSpec((3, n_track, width), lambda g: (0, 0, g)),
            pl.BlockSpec((n_epochs, n_track), lambda g: (0, 0)),
        ],
        out_specs=(
            pl.BlockSpec((3, n_epochs, width), lambda g: (0, 0, g)),
            pl.BlockSpec((3, n_knots, width), lambda g: (0, 0, g)),
        ),
        compiler_params=pltpu.CompilerParams(vmem_limit_bytes=20 << 20),
        name="geometry",
    )(gathered, fit, picks, table, look_local, means)
    return enu, spline


def solution(mesh):
    in_specs = (P("track", "ifg", "pix"), P("track", "ifg", None), P(), P(), P(None, None, "pix"))
    out_specs = (P(None, None, ("pix", "ifg", "track")), P(None, None, ("pix", "ifg", "track")))
    return jax.shard_map(shards, mesh=mesh, in_specs=in_specs, out_specs=out_specs, check_vma=False)
```

```python
import functools

import jax
import jax.numpy as jnp
from jax import lax
from jax.experimental import pallas as pl
from jax.experimental.pallas import tpu as pltpu
from jax.sharding import PartitionSpec as P

EPOCHS = 320
MESH = pl.DeviceIdType.MESH
HIGH = lax.Precision.HIGHEST
F32 = jnp.float32
BF16 = jnp.bfloat16
damping = 0.5
ridge = 0.1
BAND = 8
FIRST = 4
AHEAD_FIRST = 6
AHEAD = 2
MEAN_PIECE = 7
PAIRS_OF = ((0, 0), (0, 1), (0, 2), (1, 1), (1, 2), (2, 2))


def dot(a, b, dims=((1,), (0,)), precision=None):
    return lax.dot_general(a, b, (dims, ((), ())), precision=precision, preferred_element_type=F32)


def iota(shape, dim):
    return lax.broadcasted_iota(jnp.int32, shape, dim)


def invert_small_blocks(blocks):
    rows, lanes = blocks.shape
    state = blocks.reshape(rows // BAND, BAND, lanes)
    sub = iota(state.shape, 1)
    lane = iota(state.shape, 2) % BAND
    for k in range(BAND):
        row = state[:, k : k + 1, :]
        col = state[:, :, k : k + 1]
        inv = 1.0 / row[:, :, k : k + 1]
        scaled = row * inv
        inner = state - col * scaled
        at_row = jnp.where(lane == k, jnp.broadcast_to(inv, state.shape), jnp.broadcast_to(scaled, state.shape))
        off_row = jnp.where(lane == k, -col * inv, inner)
        state = jnp.where(sub == k, at_row, off_row)
    return state.reshape(rows, lanes)


def invert_banded(matrix):
    n = matrix.shape[0]
    lanes = 128
    row, col = iota((n, n), 0), iota((n, n), 1)
    block_row, block_col = row // BAND, col // BAND
    eye = (row == col).astype(F32)
    fold = (iota((n, lanes), 0) % BAND == iota((n, lanes), 1) % BAND).astype(F32)
    stride, inverse_diag, basis = 1, jnp.zeros((n, n), F32), eye
    while True:
        last = stride * BAND >= n
        if last:
            here_row = block_row == 0
            here_col = block_col == 0
        else:
            here_row = block_row % (2 * stride) == stride
            here_col = block_col % (2 * stride) == stride
        on_diag = here_row & here_col & (block_row == block_col)
        blocks = dot(jnp.where(on_diag, matrix, jnp.where(here_row, 0.0, eye)), fold, precision=HIGH)
        small = invert_small_blocks(blocks)
        small = jnp.concatenate([small] * (n // lanes), axis=1)
        level_inverse = jnp.where(on_diag, small, 0.0)
        inverse_diag = inverse_diag + level_inverse
        if last:
            break
        rest_row = block_row % (2 * stride) == 0
        rest_col = block_col % (2 * stride) == 0
        step = jnp.where(here_row & rest_col, dot(level_inverse, matrix, precision=HIGH), 0.0)
        matrix = jnp.where(rest_row & rest_col, matrix - dot(matrix, step, precision=HIGH), 0.0)
        basis = basis - dot(basis, step, precision=HIGH)
        stride *= 2
    scaled = dot(basis, inverse_diag, precision=HIGH)
    return dot(scaled, basis, ((1,), (1,)), precision=HIGH)


def parts(value, count):
    out = []
    for _ in range(count):
        piece = value.astype(BF16)
        out.append(piece)
        value = value - piece.astype(F32)
    return out


def spline_fitter(knots_row, n_epochs, n_knots):
    lane = iota(knots_row.shape, 1)
    before = pltpu.roll(knots_row, 1, 1)
    after = pltpu.roll(knots_row, knots_row.shape[1] - 1, 1)
    left = jnp.where(lane == 0, knots_row - 1.0, before)
    right = jnp.where(lane == n_knots - 1, knots_row + 1.0, after)
    valid = lane < n_knots
    up = jnp.where(valid, knots_row - left, 1.0)
    down = jnp.where(valid, right - knots_row, 1.0)
    epochs = iota((n_epochs, knots_row.shape[1]), 0).astype(F32)
    hat = jnp.maximum(0.0, jnp.minimum((epochs - left) / up, (right - epochs) / down))
    basis = jnp.where(valid, hat, 0.0)
    size = knots_row.shape[1]
    gram = dot(basis, basis, ((0,), (0,)), precision=HIGH)
    row, col = iota((size, size), 0), iota((size, size), 1)
    gram = jnp.where((row == col) & (row >= n_knots), 1.0, gram)
    inverse = invert_banded(gram)
    return dot(inverse[:n_knots], basis, ((1,), (1,)), precision=HIGH)


def target_of(me, k, n):
    if n != 4:
        return lax.rem(me + k + 1, n)
    half = jnp.minimum(me, 3 - me)
    near = (1 - half) if k == 0 else k + 1
    return jnp.where(me < 2, near, 3 - near)


def exchange_kernel(
    sizes, phases, pairs, date_map, knots, look,
    gathered, fit, picks, table, look_out, mean_out,
    pair_all, own, landed, weights, incid, series, sums, totals, means, look_rows,
    go, ready, own_sem, pair_send, pair_recv, look_sem, sum_send, sum_recv, total_send, total_recv, mean_send, mean_recv, z_send, z_recv, y_send, y_recv,
):
    n_track, n_ifg, n_pix, widths, n_dates, n_epochs, n_knots = sizes
    first, ahead_first, ahead, mean_piece = FIRST, AHEAD_FIRST, AHEAD, min(MEAN_PIECE, n_track * len(widths) - 5)
    track, ifg, pix = lax.axis_index("track"), lax.axis_index("ifg"), lax.axis_index("pix")
    count, pixels = phases.shape[1], phases.shape[2]
    quarter = pixels // n_ifg
    final = quarter // n_track
    padded = 8 * -(-n_dates // 8)
    while padded & (padded - 1):
        padded += 8
    padded = max(padded, 128)

    ifg_target = [target_of(ifg, k, n_ifg) for k in range(n_ifg - 1)]
    steps = sorted(range(1, n_track), key=lambda k: -min(k, n_track - k))
    track_target = [lax.rem(track + k, n_track) for k in steps]
    parts_order = track_target + [track]

    middle, helper = 1, 0
    others = [i for i in range(n_ifg) if i != middle]
    is_middle = ifg == middle
    barrier = pltpu.get_barrier_semaphore()

    @pl.when(is_middle)
    def _():
        pl.semaphore_wait(barrier, n_ifg - 1)
        for i in others:
            pl.semaphore_signal(go, inc=1, device_id={"ifg": i}, device_id_type=MESH)

    @pl.when(jnp.logical_not(is_middle))
    def _():
        pl.semaphore_signal(barrier, inc=1, device_id={"ifg": middle}, device_id_type=MESH)
        pl.semaphore_wait(go, 1)
        for k in range(n_track - 1):
            pl.semaphore_signal(barrier, inc=1, device_id={"track": track_target[k]}, device_id_type=MESH)
        for k in range(1, n_pix):
            pl.semaphore_signal(barrier, inc=1, device_id={"pix": lax.rem(pix + k, n_pix)}, device_id_type=MESH)

    def wait_for_peers():
        @pl.when(jnp.logical_not(is_middle))
        def _():
            pl.semaphore_wait(barrier, n_track + n_pix - 2)

        @pl.when(ifg == helper)
        def _():
            pl.semaphore_signal(ready, inc=1, device_id={"ifg": middle}, device_id_type=MESH)

        @pl.when(is_middle)
        def _():
            pl.semaphore_wait(ready, 1)

    own_copy = pltpu.make_async_copy(phases.at[0], own, own_sem)
    own_copy.start()
    pair_copies = []
    for k in range(n_ifg - 1):
        pair_copies.append(pltpu.make_async_remote_copy(
            src_ref=pairs.at[0], dst_ref=pair_all.at[ifg], send_sem=pair_send.at[k], recv_sem=pair_recv.at[ifg],
            device_id={"ifg": ifg_target[k]}, device_id_type=MESH))
        pair_copies[-1].start()
    pltpu.make_async_copy(pairs.at[0], pair_all.at[ifg], pair_recv.at[ifg]).start()
    look_at = pl.multiple_of(ifg * quarter + track * final, final)
    look_in = pltpu.make_async_copy(look.at[:, :, pl.ds(look_at, final)], look_rows, look_sem.at[0])
    look_in.start()
    starts = [sum(widths[:j]) for j in range(len(widths))]

    tail = max(len(widths) - 2, 0)
    order = [(j, k) for j in range(tail) for k in range(n_track)]
    order += [(j, k) for k in range(n_track) for j in range(tail, len(widths))]

    def send_piece(j, k):
        at, width, part = starts[j], widths[j], parts_order[k]
        here = pl.ds(n_track * at + k * width, width)
        for i in range(n_ifg - 1):
            start = pl.multiple_of(ifg_target[i] * quarter + part * final + at, 128)
            pltpu.make_async_remote_copy(
                src_ref=phases.at[0, :, pl.ds(start, width)], dst_ref=landed.at[ifg, :, here],
                send_sem=z_send.at[i, j, k], recv_sem=z_recv.at[ifg, j, k],
                device_id={"ifg": ifg_target[i]}, device_id_type=MESH).start()
        start = pl.multiple_of(ifg * quarter + part * final + at, 128)
        pltpu.make_async_copy(
            phases.at[0, :, pl.ds(start, width)], landed.at[ifg, :, here], z_recv.at[ifg, j, k]).start()

    ends = [sum(widths[j] for j, _ in order[: p + 1]) for p in range(len(order))]
    queued = [0]

    def send_upto(reach):
        while queued[0] < len(order) and ends[queued[0]] <= reach:
            send_piece(*order[queued[0]])
            queued[0] += 1

    send_upto(first * final // 4)

    own_copy.wait()
    piece = 1024 if pixels % 1024 == 0 else pixels
    ones = jnp.ones((8, piece), BF16)

    def add_piece(k, total):
        return total + dot(ones, own[:, pl.ds(pl.multiple_of(k * piece, piece), piece)], ((1,), (1,)))

    own_sum = lax.fori_loop(0, pixels // piece, add_piece, jnp.zeros((8, count), F32))
    sums[0] = own_sum[:1]

    code = jnp.zeros((n_epochs, 1), jnp.int32)
    for t in range(n_track):
        hit = (iota((n_epochs, n_dates), 0) == date_map[t : t + 1, :]).astype(F32)
        code = code + (jnp.max(hit, axis=1, keepdims=True) > 0.5).astype(jnp.int32) * (1 << t)
    n_masks = 1 << n_track
    lane = iota((n_epochs, 3 * n_masks), 1)
    picks[...] = (lane % n_masks == code).astype(F32).astype(BF16)

    knots_row = jnp.concatenate([knots[...], jnp.zeros((1, 128 - n_knots), jnp.int32)], axis=1).astype(F32)
    fitter = spline_fitter(knots_row, n_epochs, n_knots)
    high, low = parts(fitter, 2)
    fit[...] = jnp.concatenate(
        [jnp.concatenate([high, high], axis=1), jnp.concatenate([low, jnp.zeros_like(low)], axis=1)], axis=0)

    look_in.wait()
    look_out[...] = look_rows[...]
    mask = iota((n_masks, final), 0)
    bits = [((mask >> t) & 1).astype(F32) for t in range(n_track)]

    def entry(i, j):
        value = ridge if i == j else 0.0
        for t in range(n_track):
            value = value + bits[t] * (look_rows[i, t : t + 1, :] * look_rows[j, t : t + 1, :])
        return value

    a00, a01, a02, a11, a12, a22 = [entry(i, j) for i, j in PAIRS_OF]
    c00 = a11 * a22 - a12 * a12
    c01 = a02 * a12 - a01 * a22
    c02 = a01 * a12 - a02 * a11
    c11 = a00 * a22 - a02 * a02
    c12 = a01 * a02 - a00 * a12
    c22 = a00 * a11 - a01 * a01
    det = a00 * c00 + a01 * c01 + a02 * c02
    for e, cofactor in enumerate((c00, c01, c02, c11, c12, c22)):
        table[e] = jnp.concatenate(parts(cofactor / det, 3), axis=0)

    wait_for_peers()
    sum_copies = []
    for k in range(1, n_pix):
        sum_copies.append(pltpu.make_async_remote_copy(
            src_ref=sums.at[0], dst_ref=sums.at[k], send_sem=sum_send.at[k], recv_sem=sum_recv.at[k],
            device_id={"pix": lax.rem(pix + k, n_pix)}, device_id_type=MESH))
        sum_copies[-1].start()
    send_upto(ahead_first * final // 4)

    for s in range(n_ifg):
        pltpu.make_async_copy(pair_all.at[s], pair_all.at[s], pair_recv.at[s]).wait()
    normal = jnp.zeros((padded, padded), F32)
    dates = iota((padded, count), 0)
    for s in range(n_ifg):
        rows = pair_all[s]
        matrix = (dates == rows[1:2, :]).astype(F32) - (dates == rows[0:1, :]).astype(F32)
        incid[s] = matrix
        matrix = matrix.astype(BF16)
        normal = normal + dot(matrix, matrix, ((1,), (1,)))
    normal = normal + jnp.where(iota(normal.shape, 0) == iota(normal.shape, 1), damping, 0.0)
    inverse = invert_banded(normal)

    total = sums[0]
    for k in range(1, n_pix):
        pltpu.make_async_copy(sums.at[k], sums.at[k], sum_recv.at[k]).wait()
        total = total + sums[k]
    totals[ifg] = total

    my_map = date_map[pl.ds(track, 1), :]
    placed = (iota((n_epochs, n_dates), 0) == my_map).astype(F32)
    placed = dot(placed, inverse[:n_dates], precision=HIGH)
    for s in range(n_ifg):
        weight = dot(placed, incid[s], precision=HIGH)
        weights[s, 0], weights[s, 1] = parts(weight, 2)
    total_copies = []
    for k in range(n_ifg - 1):
        total_copies.append(pltpu.make_async_remote_copy(
            src_ref=totals.at[ifg], dst_ref=totals.at[ifg], send_sem=total_send.at[k], recv_sem=total_recv.at[ifg],
            device_id={"ifg": ifg_target[k]}, device_id_type=MESH))
        total_copies[-1].start()

    def send_mean():
        for k in range(n_ifg - 1):
            s = ifg_target[k]
            pltpu.make_async_copy(totals.at[s], totals.at[s], total_recv.at[s]).wait()
        mean = jnp.zeros((1, n_epochs), F32)
        for s in range(n_ifg):
            weight = weights[s, 0].astype(F32) + weights[s, 1].astype(F32)
            mean = mean + dot(totals[s], weight, ((1,), (1,)), precision=HIGH)
        means[track] = mean / (pixels * n_pix)
        for k in range(n_track - 1):
            mean_copies.append(pltpu.make_async_remote_copy(
                src_ref=means.at[track], dst_ref=means.at[track], send_sem=mean_send.at[k], recv_sem=mean_recv.at[track],
                device_id={"track": track_target[k]}, device_id_type=MESH))
            mean_copies[-1].start()

    mean_copies = []
    def mean_columns():
        for k in range(n_track - 1):
            t = track_target[k]
            pltpu.make_async_copy(means.at[t], means.at[t], mean_recv.at[t]).wait()
        eye = (iota((n_epochs, n_epochs), 0) == iota((n_epochs, n_epochs), 1)).astype(F32)
        mean_out[...] = jnp.concatenate(
            [dot(eye, means[t], ((1,), (1,)), precision=HIGH) for t in range(n_track)], axis=1)

    for at_piece, (j, k) in enumerate(order):
        at, width, part = starts[j], widths[j], parts_order[k]
        if at_piece == mean_piece:
            send_mean()
        if at_piece == max(len(order) - 4, mean_piece + 1):
            mean_columns()
        here = pl.ds(n_track * at + k * width, width)
        for s in range(n_ifg):
            chunk = landed.at[s, :, here]
            pltpu.make_async_copy(chunk, chunk, z_recv.at[s, j, k]).wait()
        send_upto(n_track * final if at_piece == len(order) - 1 else ends[at_piece] + ahead * final // 4)
        value = jnp.zeros((n_epochs, width), F32)
        for s in range(n_ifg):
            phase = landed[s, :, here]
            value = value + dot(weights[s, 0], phase) + dot(weights[s, 1], phase)
        series[:, here] = value
        if k < n_track - 1:
            pltpu.make_async_remote_copy(
                src_ref=series.at[:, here], dst_ref=gathered.at[track, :, pl.ds(at, width)],
                send_sem=y_send.at[k, j], recv_sem=y_recv.at[track, j],
                device_id={"track": part}, device_id_type=MESH).start()
        else:
            pltpu.make_async_copy(
                series.at[:, here], gathered.at[track, :, pl.ds(at, width)], y_recv.at[track, j]).start()

    for copy in pair_copies + sum_copies + total_copies + mean_copies:
        copy.wait_send()
    at = 0
    for j, width in enumerate(widths):
        for i in range(n_ifg - 1):
            for k in range(n_track):
                chunk = landed.at[0, :, pl.ds(0, width)]
                pltpu.make_async_copy(chunk, chunk, z_send.at[i, j, k]).wait()
        for t in range(n_track):
            here = gathered.at[t, :, pl.ds(at, width)]
            pltpu.make_async_copy(here, here, y_recv.at[t, j]).wait()
        for k in range(n_track - 1):
            here = series.at[:, pl.ds(0, width)]
            pltpu.make_async_copy(here, here, y_send.at[k, j]).wait()
        at += width


def geometry_kernel(gathered, fit, picks, table, look, means, enu, spline):
    n_track = gathered.shape[0]
    select = picks[...]
    entries = {}
    for e, (i, j) in enumerate(PAIRS_OF):
        entries[i, j] = entries[j, i] = dot(select, table[e])
    tracks = [gathered[t] - means[:, t : t + 1] for t in range(n_track)]
    right = []
    for i in range(3):
        value = look[i, 0:1, :] * tracks[0]
        for t in range(1, n_track):
            value = value + look[i, t : t + 1, :] * tracks[t]
        right.append(value)
    for i in range(3):
        value = entries[i, 0] * right[0] + entries[i, 1] * right[1] + entries[i, 2] * right[2]
        enu[i] = value
        both = dot(fit[...], jnp.concatenate(parts(value, 2), axis=0))
        spline[i] = both[: both.shape[0] // 2] + both[both.shape[0] // 2 :]


def stay(value):
    return pltpu.with_memory_space_constraint(value, pltpu.HBM)


def chunk_widths(final):
    if final == 1024:
        return (256, 256, 256, 128, 128)
    return (final // 2, final // 2) if final % 256 == 0 else (final,)


def shards(phases, pairs, date_map, knots, look):
    n_track, n_ifg, n_pix = lax.axis_size("track"), lax.axis_size("ifg"), lax.axis_size("pix")
    count, pixels = phases.shape[1], phases.shape[2]
    quarter = pixels // n_ifg
    final = quarter // n_track
    n_dates, n_epochs, n_knots = date_map.shape[1], EPOCHS, knots.shape[0]
    widths = chunk_widths(final)
    n = len(widths)
    padded = 128
    while padded < n_dates:
        padded *= 2
    n_masks = 1 << n_track
    sizes = (n_track, n_ifg, n_pix, widths, n_dates, n_epochs, n_knots)
    vmem = pl.BlockSpec(memory_space=pltpu.VMEM)
    anywhere = pl.BlockSpec(memory_space=pl.ANY)
    outside = pl.BlockSpec(memory_space=pltpu.HBM)
    dma = pltpu.SemaphoreType.DMA
    gathered, fit, picks, table, look_local, means = pl.pallas_call(
        functools.partial(exchange_kernel, sizes),
        out_shape=(
            jax.ShapeDtypeStruct((n_track, n_epochs, final), F32),
            jax.ShapeDtypeStruct((2 * n_knots, 2 * n_epochs), BF16),
            jax.ShapeDtypeStruct((n_epochs, 3 * n_masks), BF16),
            jax.ShapeDtypeStruct((len(PAIRS_OF), 3 * n_masks, final), BF16),
            jax.ShapeDtypeStruct((3, n_track, final), F32),
            jax.ShapeDtypeStruct((n_epochs, n_track), F32),
        ),
        in_specs=[outside, outside, vmem, vmem, outside],
        out_specs=(anywhere,) + (vmem,) * 5,
        scratch_shapes=[
            pltpu.VMEM((n_ifg, 2, count), jnp.int32),
            pltpu.VMEM((count, pixels), BF16),
            pltpu.VMEM((n_ifg, count, quarter), BF16),
            pltpu.VMEM((n_ifg, 2, n_epochs, count), BF16),
            pltpu.VMEM((n_ifg, padded, count), F32),
            pltpu.VMEM((n_epochs, quarter), F32),
            pltpu.VMEM((n_pix, 1, count), F32),
            pltpu.VMEM((n_ifg, 1, count), F32),
            pltpu.VMEM((n_track, 1, n_epochs), F32),
            pltpu.VMEM((3, n_track, final), F32),
            pltpu.SemaphoreType.REGULAR, pltpu.SemaphoreType.REGULAR,
            dma(()), dma((n_ifg,)), dma((n_ifg,)), dma((1,)),
            dma((n_pix,)), dma((n_pix,)), dma((n_ifg,)), dma((n_ifg,)),
            dma((n_track,)), dma((n_track,)), dma((n_ifg, n, n_track)), dma((n_ifg, n, n_track)), dma((n_track, n)), dma((n_track, n)),
        ],
        compiler_params=pltpu.CompilerParams(collective_id=0, has_side_effects=True, vmem_limit_bytes=28 << 20),
        name="exchange",
    )(stay(phases), stay(jnp.transpose(pairs, (0, 2, 1))), stay(date_map), stay(knots[None, :]), stay(jnp.transpose(look, (1, 0, 2))))
    width = min(final, 256)
    enu, spline = pl.pallas_call(
        geometry_kernel,
        grid=(final // width,),
        out_shape=(
            jax.ShapeDtypeStruct((3, n_epochs, final), F32),
            jax.ShapeDtypeStruct((3, n_knots, final), F32),
        ),
        in_specs=[
            pl.BlockSpec((n_track, n_epochs, width), lambda g: (0, 0, g)),
            pl.BlockSpec((2 * n_knots, 2 * n_epochs), lambda g: (0, 0)),
            pl.BlockSpec((n_epochs, 3 * n_masks), lambda g: (0, 0)),
            pl.BlockSpec((len(PAIRS_OF), 3 * n_masks, width), lambda g: (0, 0, g)),
            pl.BlockSpec((3, n_track, width), lambda g: (0, 0, g)),
            pl.BlockSpec((n_epochs, n_track), lambda g: (0, 0)),
        ],
        out_specs=(
            pl.BlockSpec((3, n_epochs, width), lambda g: (0, 0, g)),
            pl.BlockSpec((3, n_knots, width), lambda g: (0, 0, g)),
        ),
        compiler_params=pltpu.CompilerParams(vmem_limit_bytes=20 << 20),
        name="geometry",
    )(gathered, fit, picks, table, look_local, means)
    return enu, spline


def solution(mesh):
    in_specs = (P("track", "ifg", "pix"), P("track", "ifg", None), P(), P(), P(None, None, "pix"))
    out_specs = (P(None, None, ("pix", "ifg", "track")), P(None, None, ("pix", "ifg", "track")))
    return jax.shard_map(shards, mesh=mesh, in_specs=in_specs, out_specs=out_specs, check_vma=False)
```
